256 devices in a mesh: seq: 64 (over y, z, core), head: 4 (over x).
Axes of the slice: x: 4, y: 4, z: 8, core: 2. Of those that a mesh axis runs over, the one named last changes fastest.
Arguments:
- queries: bfloat16 [32768, 2048], P('seq', 'head'), may hold values from -6 to 6
- keys: bfloat16 [32768, 2048], P('seq', 'head'), may hold values from -6 to 6
- values: bfloat16 [32768, 4096], P('seq', 'head'), may hold values from -6 to 6
- forget_gate: float32 [32768, 8], P('seq', 'head'), may hold values from -1 to 14
- input_gate: float32 [32768, 8], P('seq', 'head'), may hold values from -5 to 215
- out_weight: bfloat16 [4096, 4096], P('head'), may hold values from -0.125 to 0.125
Outputs:
- mixed: bfloat16 [32768, 4096], P('seq', 'head')
- gate_mean: float32 [8], P('head')
The draws below stay inside these ranges and needn't reach their ends.
All inputs are finite; a program needn't handle non-finite values.
Results may differ from the reference program's by a relative error of at most 0.01.
Values may be sent and summed in bfloat16 or wider, within the bound.
A program may use at most 192 MiB of HBM per device.

```python
import math
import jax
import jax.numpy as jnp
from jax import lax

D = 4096
HEAD_TOTAL = 8
DQK = 256
DV = 512
TOK_DEV = 512
SEQUENCE_TOKENS = 32768
N_HEAD = 4


def draw_forget_gate(key, part):
    starting_key = jax.random.fold_in(key, 101)
    key_for_shuffle, key_for_token, key_for_block, key_for_spike, key_magnitude = jax.random.split(starting_key, 5)
    head_order = jax.random.permutation(key_for_shuffle, HEAD_TOTAL)
    keep_count = HEAD_TOTAL // 2
    slow_heads = head_order < keep_count
    starting_rate = jnp.where(slow_heads, math.log(10.0) / (4.0 * SEQUENCE_TOKENS), 1.0 / 40.0).astype(jnp.float32)
    token_multiplier = jnp.exp(jax.random.uniform(key_for_token, (SEQUENCE_TOKENS, HEAD_TOTAL), jnp.float32, -0.6931, 0.6931))
    block_count = SEQUENCE_TOKENS // TOK_DEV
    block_multiplier = jnp.exp(jax.random.uniform(key_for_block, (block_count, HEAD_TOTAL), jnp.float32, -0.6931, 0.6931))
    block_multiplier = jnp.repeat(block_multiplier, TOK_DEV, axis=0)
    spike_mask = jax.random.uniform(key_for_spike, (SEQUENCE_TOKENS, HEAD_TOTAL), jnp.float32) < 3.0 / SEQUENCE_TOKENS
    spike_magnitude = jax.random.uniform(key_magnitude, (SEQUENCE_TOKENS, HEAD_TOTAL), jnp.float32, 0.2231, 0.6931)
    forget_rate = starting_rate[None, :] * token_multiplier * block_multiplier + jnp.where(spike_mask, spike_magnitude, 0.0)
    return (-jnp.log(jnp.expm1(forget_rate))).astype(jnp.float32)


def draw_input_gate(key, part):
    starting_key = jax.random.fold_in(key, 202)
    key_noise = jax.random.fold_in(starting_key, 0)
    position_ramp = (jnp.arange(SEQUENCE_TOKENS).astype(jnp.float32) / SEQUENCE_TOKENS)[:, None]
    jitter = jnp.clip(jax.random.normal(key_noise, (SEQUENCE_TOKENS, HEAD_TOTAL), jnp.float32), -4.0, 4.0)
    result = 1.0 + 2.0 * position_ramp + jitter
    return result.astype(jnp.float32)


def with_spikes(array, own_key, source, target, blocks, factor):
    def block_of(dim):
        return (jnp.arange(array.shape[dim]) // (array.shape[dim] // blocks)).reshape((-1,) + (1,) * (array.ndim - 1 - dim))

    near = jax.random.permutation(own_key, blocks)[block_of(target)]
    other_side = (block_of(target) + blocks // 2) % blocks
    return jnp.where((block_of(source) == near) | (block_of(source) == other_side), factor * array, array)


def levels(key, dims, cuts, smallest, largest):
    level, own = 1.0, jax.random.fold_in(key, 6)
    for position, blocks in cuts:
        steps = jnp.exp(jax.random.uniform(jax.random.fold_in(own, position), (blocks,), jnp.float32, smallest / len(cuts), largest / len(cuts)))
        level = level * jnp.repeat(steps, dims[position] // blocks).reshape([-1 if axis == position else 1 for axis in range(len(dims))])
    return level


def bell_draw(key, dims, scale, reach, shards=(), kind=jnp.bfloat16):
    drawn = jax.random.normal(key, dims, jnp.float32) * scale
    if len(shards) > 0:
        drawn = levels(key, dims, shards, -0.22, 0.18) * drawn
    return jnp.clip(drawn, min=-reach, max=reach).astype(kind)


def gaussian_with(rng, dims, width, most, cuts, heavy, kind=jnp.bfloat16):
    values = width * jax.random.normal(rng, dims, jnp.float32)
    if cuts:
        values = values * levels(rng, dims, cuts, -0.22, 0.18)
    return jnp.clip(with_spikes(values, jax.random.fold_in(rng, 3), *heavy), -most, most).astype(kind)


def setup_inputs(seed: int = 0) -> dict:
    splits = jax.random.split(jax.random.key(seed), 7)
    return {
        "queries": bell_draw(splits[0], (SEQUENCE_TOKENS, HEAD_TOTAL * DQK), 1.0, 6.0, ((0, 64), (1, 4))),
        "keys": bell_draw(splits[1], (SEQUENCE_TOKENS, HEAD_TOTAL * DQK), 1.0, 6.0, ((0, 64), (1, 4))),
        "values": bell_draw(splits[2], (SEQUENCE_TOKENS, HEAD_TOTAL * DV), 1.0, 6.0, ((0, 64), (1, 4))),
        "forget_gate": draw_forget_gate(jax.random.fold_in(splits[6], 71), 0),
        "input_gate": draw_input_gate(jax.random.fold_in(splits[6], 71), 0),
        "out_weight": gaussian_with(splits[5], (HEAD_TOTAL * DV, D), (HEAD_TOTAL * DV) ** -0.5, 0.125, ((0, 4),), (0, 1, 4, 2.0)),
    }


def combine_states(earlier, later_state):
    e_matrix, e_norm, e_max, e_decay = earlier
    l_matrix, l_norm, l_max, l_decay = later_state
    merged_max = jnp.maximum(l_decay + e_max, l_max)
    e_scale = jnp.exp(l_decay + e_max - merged_max)
    l_scale = jnp.exp(l_max - merged_max)
    return (e_scale[:, None, None] * e_matrix + l_scale[:, None, None] * l_matrix, e_scale[:, None] * e_norm + l_scale[:, None] * l_norm, merged_max, e_decay + l_decay)

def intra_terms(q_heads, k_heads, v_heads, cum_decay, input_block):
    length = q_heads.shape[0]
    positions = jnp.arange(length)
    causal = positions[:, None] >= positions[None, :]
    log_weight = cum_decay.T[:, :, None] - cum_decay.T[:, None, :] + input_block.T[:, None, :]
    log_weight = jnp.where(causal[None], log_weight, -jnp.inf)
    intra_max = lax.optimization_barrier(jnp.max(log_weight, axis=2))
    factors = jnp.exp(log_weight - intra_max[:, :, None])
    scores = jnp.einsum('thd,shd->hts', q_heads.astype(jnp.float32), k_heads.astype(jnp.float32)) / math.sqrt(q_heads.shape[2])
    weighted = factors * scores
    intra_den = lax.optimization_barrier(jnp.sum(weighted, axis=2))
    rounded_weights = lax.optimization_barrier(weighted.astype(jnp.bfloat16))
    intra_num = jnp.einsum('hts,shv->thv', rounded_weights.astype(jnp.float32), v_heads.astype(jnp.float32))
    return (intra_num, intra_den, intra_max)

def own_terms(k_heads, v_heads, cum_decay, input_block):
    block_decay = cum_decay[-1]
    own_log = block_decay[None, :] - cum_decay + input_block
    own_max = lax.optimization_barrier(jnp.max(own_log, axis=0))
    key_weight = jnp.exp(own_log - own_max[None, :]) / math.sqrt(k_heads.shape[2])
    weighted_keys = k_heads.astype(jnp.float32) * key_weight[:, :, None]
    own_norm = lax.optimization_barrier(jnp.sum(weighted_keys, axis=0))
    rounded_keys = lax.optimization_barrier(weighted_keys.astype(jnp.bfloat16))
    own_matrix = jnp.einsum('shv,shk->hvk', v_heads.astype(jnp.float32), rounded_keys.astype(jnp.float32))
    return (own_matrix, own_norm, own_max, block_decay)

def readout(intra, carried_state, q_heads, cum_decay):
    intra_num, intra_den, intra_max = intra
    carry_matrix, carry_norm, carry_max, unused_decay = carried_state
    carried_log = cum_decay.T + carry_max[:, None]
    stabilizer = jnp.maximum(intra_max, carried_log)
    intra_scale = jnp.exp(intra_max - stabilizer).T
    carry_scale = jnp.exp(carried_log - stabilizer).T
    q_float = q_heads.astype(jnp.float32)
    carried_num = jnp.einsum('hvk,thk->thv', carry_matrix, q_float, precision=lax.Precision.HIGHEST)
    carried_den = jnp.einsum('hk,thk->th', carry_norm, q_float, precision=lax.Precision.HIGHEST)
    numerator = intra_scale[:, :, None] * intra_num + carry_scale[:, :, None] * carried_num
    denominator = intra_scale * intra_den.T + carry_scale * carried_den
    return (numerator / jnp.maximum(jnp.abs(denominator), 1.0)[:, :, None]).astype(jnp.bfloat16)

def reference(queries, keys, values, forget_gate, input_gate, out_weight):
    block_count = SEQUENCE_TOKENS // TOK_DEV
    group_width = HEAD_TOTAL * DV // N_HEAD
    q_blocks = queries.reshape(block_count, TOK_DEV, HEAD_TOTAL, DQK)
    k_blocks = keys.reshape(block_count, TOK_DEV, HEAD_TOTAL, DQK)
    v_blocks = values.reshape(block_count, TOK_DEV, HEAD_TOTAL, DV)
    f_blocks = forget_gate.reshape(block_count, TOK_DEV, HEAD_TOTAL)
    i_blocks = input_gate.reshape(block_count, TOK_DEV, HEAD_TOTAL)

    def block_step(carried_state, block_inputs):
        q_heads, k_heads, v_heads, forget_block, input_block = block_inputs
        cum_decay = jnp.cumsum(jax.nn.log_sigmoid(forget_block), axis=0)
        intra = intra_terms(q_heads, k_heads, v_heads, cum_decay, input_block)
        own_state = own_terms(k_heads, v_heads, cum_decay, input_block)
        hidden = readout(intra, carried_state, q_heads, cum_decay).reshape(TOK_DEV, HEAD_TOTAL * DV)
        summed = jnp.zeros((TOK_DEV, D), jnp.float32)
        for group_index in range(N_HEAD):
            lower = group_index * group_width
            partial_value = jnp.dot(hidden[:, lower:lower + group_width], out_weight[lower:lower + group_width, :], preferred_element_type=jnp.float32)
            partial_value = lax.optimization_barrier(partial_value.astype(jnp.bfloat16))
            summed = summed + partial_value.astype(jnp.float32)
        return (combine_states(carried_state, own_state), summed.astype(jnp.bfloat16))
    start_state = (jnp.zeros((HEAD_TOTAL, DV, DQK), jnp.float32), jnp.zeros((HEAD_TOTAL, DQK), jnp.float32), jnp.full((HEAD_TOTAL,), -1e+30, jnp.float32), jnp.zeros((HEAD_TOTAL,), jnp.float32))
    unused_state, mixed_blocks = lax.scan(block_step, start_state, (q_blocks, k_blocks, v_blocks, f_blocks, i_blocks))
    mixed = mixed_blocks.reshape(SEQUENCE_TOKENS, D)
    gate_mean = lax.optimization_barrier(jnp.mean(input_gate, axis=0))
    return (mixed, gate_mean)
```

```python
import functools

import jax
import jax.numpy as jnp
from jax import lax
from jax.experimental import pallas as pl
from jax.experimental.pallas import tpu as pltpu
from jax.sharding import Mesh
from jax.sharding import PartitionSpec as P

MESH = pl.DeviceIdType.MESH
SEQ = ("y", "z", "c")
F32 = jnp.float32
BF16 = jnp.bfloat16
LOW = -1e30
INFO = 640


def dot(a, b):
    return jnp.dot(a, b, preferred_element_type=F32)


def merge(e_max, l_max, l_decay):
    top = jnp.maximum(l_decay + e_max, l_max)
    return jnp.exp(l_decay + e_max - top), jnp.exp(l_max - top), top


def three_rows(row, first):
    hi = row.astype(BF16).astype(F32)
    mid = (row - hi).astype(BF16).astype(F32)
    low = row - hi - mid
    return jnp.where(first == 0, hi, jnp.where(first == 1, mid, jnp.where(first == 2, low, 0.0))).astype(BF16)


def read_info(ref, j):
    row = ref[j]
    return row[:, :256], row[:, 256:257], row[:, 384:385], row[:, 512:513]


def write_info(ref, norm, top, decay, gate):
    ref[0, :, 0:256] = norm
    ref[0, :, 256:384] = jnp.broadcast_to(top, (1, 128))
    ref[0, :, 384:512] = jnp.broadcast_to(decay, (1, 128))
    ref[0, :, 512:640] = jnp.broadcast_to(gate, (1, 128))


def kernel(
    sizes,
    q_hbm, k_hbm, v_hbm, fg_hbm, ig_hbm, w_hbm,
    mixed_hbm, gate_ref,
    q_buf, k_buf, v_buf, fg_buf, ig_buf, w_buf, kt_buf,
    own1, pair_out, pair_in, pinfo_out, pinfo_in,
    t_buf, t_in, tinfo_out, tinfo,
    p_buf, y_out, y_in, yinfo_out, yinfo,
    e_buf, e_in, f_out, f_in, finfo_out, finfo_in, mine,
    num_buf, bmax_buf, den_buf, hid,
    s1_out, s1_in, dir_out, dir_in, rel_out, rel_in, own_p, rel_p, out_buf,
    load_sem, w_sem, out_sem,
    pair_ss, pair_rs, z_ss, z_rs, zi_ss, zi_rs, y_ss, y_rs, yi_ss, yi_rs, e_ss, e_rs, f_ss, f_rs,
    s1_ss, s1_rs, dir_ss, dir_rs, rel_ss, rel_rs,
):
    ny, nz, nx = sizes
    y, z, c, x = (lax.axis_index(a) for a in ("y", "z", "c", "x"))
    tokens = q_buf.shape[1]
    dk, dv = q_buf.shape[2], v_buf.shape[2]
    half = tokens // 2
    cols = w_buf.shape[2]
    share = dk // nz
    first = c == 0
    heads = (1 - c, c)

    loads = []

    def load(src, dst):
        copy = pltpu.make_async_copy(src, dst, load_sem.at[len(loads)])
        copy.start()
        loads.append(copy)

    load(fg_hbm, fg_buf)
    load(ig_hbm, ig_buf)
    for s in range(2):
        load(k_hbm.at[:, pl.ds(pl.multiple_of(heads[s] * dk, 128), dk)], k_buf.at[s])
        load(v_hbm.at[:, pl.ds(pl.multiple_of(heads[s] * dv, 128), dv)], v_buf.at[s])
    for s in range(2):
        load(q_hbm.at[:, pl.ds(pl.multiple_of(heads[s] * dk, 128), dk)], q_buf.at[s])

    barrier = pltpu.get_barrier_semaphore()
    peers = [{"c": 1 - c}]
    peers += [{"z": lax.rem(z + d, nz)} for d in range(1, nz)]
    peers += [{"y": lax.rem(y + d, ny)} for d in range(1, ny)]
    left, right = {"x": lax.rem(x + nx - 1, nx)}, {"x": lax.rem(x + 1, nx)}
    peers += [left, right]
    for peer in peers:
        pl.semaphore_signal(barrier, inc=1, device_id=peer, device_id_type=MESH)

    targets = (lax.rem(x + 2, nx), lax.rem(x + nx - 1, nx), lax.rem(x + 1, nx), x)
    w_loads = []
    for i in range(4):
        for s in range(2):
            copy = pltpu.make_async_copy(
                w_hbm.at[pl.ds(pl.multiple_of(heads[s] * dv, 128), dv), pl.ds(pl.multiple_of(targets[i] * cols, 128), cols)],
                w_buf.at[i, pl.ds(s * dv, dv), :],
                w_sem.at[2 * i + s],
            )
            copy.start()
            w_loads.append(copy)

    loads[0].wait()
    loads[1].wait()
    fg, ig = fg_buf[...], ig_buf[...]
    lf = jnp.minimum(fg, 0.0) - jnp.log1p(jnp.exp(-jnp.abs(fg)))
    lf_rows = (jnp.where(first, lf[1:2], lf[0:1]), jnp.where(first, lf[0:1], lf[1:2]))
    ig_rows = (jnp.where(first, ig[1:2], ig[0:1]), jnp.where(first, ig[0:1], ig[1:2]))
    sub = lax.broadcasted_iota(jnp.int32, (8, tokens), 0)
    upper = (
        lax.broadcasted_iota(jnp.int32, (tokens, tokens), 0) <= lax.broadcasted_iota(jnp.int32, (tokens, tokens), 1)
    ).astype(F32).astype(BF16)
    stacked = jnp.where(
        sub < 4,
        three_rows(jnp.broadcast_to(lf_rows[0], (8, tokens)), sub).astype(F32),
        three_rows(jnp.broadcast_to(lf_rows[1], (8, tokens)), sub - 4).astype(F32),
    ).astype(BF16)
    cums = dot(stacked, upper)
    b_rows, decays, tops, weights = [], [], [], []
    for s in range(2):
        cum = jnp.sum(cums[4 * s : 4 * s + 4], axis=0, keepdims=True)
        b = ig_rows[s] - cum
        decay = cum[:, tokens - 1 : tokens]
        b_top = jnp.max(b, axis=1, keepdims=True)
        b_rows.append(b)
        decays.append(decay)
        tops.append(decay + b_top)
        weights.append(jnp.exp(b - b_top) * (dk**-0.5))
    gates = [jnp.sum(ig_rows[s], axis=1, keepdims=True) for s in range(2)]

    def own_state(s):
        kt = k_buf[s].T
        kt_buf[s] = kt
        wkt = (kt.astype(F32) * weights[s]).astype(BF16)
        matrix = dot(wkt, v_buf[s])
        norm = jnp.sum(dot(three_rows(jnp.broadcast_to(weights[s], (8, tokens)), sub), k_buf[s]), axis=0, keepdims=True)
        return matrix, norm

    def remote(src, dst, ss, rs, peer):
        return pltpu.make_async_remote_copy(
            src_ref=src, dst_ref=dst, send_sem=ss, recv_sem=rs, device_id=peer, device_id_type=MESH
        )

    sends = []

    loads[2].wait()
    loads[3].wait()
    matrix0, norm0 = own_state(0)
    pair_out[...] = matrix0.astype(BF16)
    write_info(pinfo_out, norm0, tops[0], decays[0], gates[0])
    pl.semaphore_wait(barrier, len(peers))
    partner = {"c": 1 - c}
    pair = [
        remote(pinfo_out, pinfo_in, pair_ss.at[0], pair_rs.at[0], partner),
        remote(pair_out, pair_in, pair_ss.at[1], pair_rs.at[1], partner),
    ]
    for copy in pair:
        copy.start()
    sends += pair

    loads[4].wait()
    loads[5].wait()
    matrix1, norm1 = own_state(1)
    own1[...] = matrix1

    pair[0].wait_recv()
    in_norm, in_top, in_decay, in_gate = read_info(pinfo_in, 0)
    a_top, a_norm = jnp.where(first, tops[1], in_top), jnp.where(first, norm1, in_norm)
    a_decay = jnp.where(first, decays[1], in_decay)
    l_top, l_norm = jnp.where(first, in_top, tops[1]), jnp.where(first, in_norm, norm1)
    l_decay = jnp.where(first, in_decay, decays[1])
    e_scale, l_scale, chip_top = merge(a_top, l_top, l_decay)
    chip_norm = e_scale * a_norm + l_scale * l_norm
    write_info(tinfo_out, chip_norm, chip_top, a_decay + l_decay, gates[1] + in_gate)
    zi = []
    order = sorted(range(1, nz), key=lambda d: -min(d, nz - d))
    for d in order:
        copy = remote(tinfo_out.at[0], tinfo.at[z], zi_ss.at[d], zi_rs.at[d], {"z": lax.rem(z + d, nz)})
        copy.start()
        zi.append(copy)
    tinfo[z] = tinfo_out[0]
    own_scale, in_scale = jnp.where(first, e_scale, l_scale), jnp.where(first, l_scale, e_scale)
    pair[1].wait_recv()
    zs = []
    for j in range(nz):
        rows = pl.ds(j * share, share)
        t_buf[j] = (own_scale * own1[rows, :] + in_scale * pair_in[rows, :].astype(F32)).astype(BF16)
    for d in order:
        peer = lax.rem(z + d, nz)
        copy = remote(t_buf.at[peer], t_in.at[z], z_ss.at[d], z_rs.at[d], {"z": peer})
        copy.start()
        zs.append(copy)
    t_in[z] = t_buf[z]
    sends += zi + zs

    loads[6].wait()
    loads[7].wait()

    def intra(s):
        for r in range(2):
            rows = pl.ds(r * half, half)
            span = half * (r + 1)
            scores = dot(q_buf[s, rows, :], kt_buf[s, :, :span]) * (dk**-0.5)
            t_index = lax.broadcasted_iota(jnp.int32, (half, span), 0) + r * half
            s_index = lax.broadcasted_iota(jnp.int32, (half, span), 1)
            logs = jnp.where(s_index <= t_index, jnp.broadcast_to(b_rows[s][:, :span], (half, span)), -jnp.inf)
            top = jnp.max(logs, axis=1, keepdims=True)
            weighted = jnp.exp(logs - top) * scores
            bmax_buf[s, rows, :] = top
            den_buf[s, rows, :] = jnp.sum(weighted, axis=1, keepdims=True)
            num_buf[s, rows, :] = dot(weighted.astype(BF16), v_buf[s, :span, :])

    intra(1)
    intra(0)

    for copy in zi:
        copy.wait_recv()
    top, decay, norm, gate = jnp.full((1, 1), LOW, F32), jnp.zeros((1, 1), F32), jnp.zeros((1, dk), F32), jnp.zeros((1, 1), F32)
    z_norm, z_top, z_decay = norm, top, decay
    z_tops, z_decays, scales = [], [], []
    for j in range(nz):
        z_tops.append(top)
        z_decays.append(decay)
        here = j == z
        z_norm, z_top, z_decay = jnp.where(here, norm, z_norm), jnp.where(here, top, z_top), jnp.where(here, decay, z_decay)
        j_norm, j_top, j_decay, j_gate = read_info(tinfo, j)
        e_scale, l_scale, top = merge(top, j_top, j_decay)
        norm = e_scale * norm + l_scale * j_norm
        decay = decay + j_decay
        gate = gate + j_gate
        scales.append((e_scale, l_scale))
    write_info(yinfo_out, norm, top, decay, gate)
    yi = []
    y_order = sorted(range(1, ny), key=lambda d: -min(d, ny - d))
    for d in y_order:
        copy = remote(yinfo_out.at[0], yinfo.at[y], yi_ss.at[d], yi_rs.at[d], {"y": lax.rem(y + d, ny)})
        copy.start()
        yi.append(copy)
    yinfo[y] = yinfo_out[0]
    for copy in zs:
        copy.wait_recv()
    running = jnp.zeros((share, dv), F32)
    for j in range(nz):
        p_buf[j] = running
        running = scales[j][0] * running + scales[j][1] * t_in[j].astype(F32)
    y_out[...] = running.astype(BF16)
    ys = []
    for d in y_order:
        copy = remote(y_out, y_in.at[y], y_ss.at[d], y_rs.at[d], {"y": lax.rem(y + d, ny)})
        copy.start()
        ys.append(copy)
    y_in[y] = y_out[...]
    sends += yi + ys

    for copy in yi:
        copy.wait_recv()
    top, decay, norm, gate = jnp.full((1, 1), LOW, F32), jnp.zeros((1, 1), F32), jnp.zeros((1, dk), F32), jnp.zeros((1, 1), F32)
    y_scales = []
    for j in range(ny):
        j_norm, j_top, j_decay, j_gate = read_info(yinfo, j)
        passed = j < y
        e_scale, l_scale, next_top = merge(top, j_top, j_decay)
        norm = jnp.where(passed, e_scale * norm + l_scale * j_norm, norm)
        top = jnp.where(passed, next_top, top)
        gate = gate + j_gate
        y_scales.append((jnp.where(passed, e_scale, 1.0), jnp.where(passed, l_scale, 0.0)))
    e_scales = [merge(top, z_tops[j], z_decays[j]) for j in range(nz)]
    e_scale, l_scale, chip_max = merge(top, z_top, z_decay)
    enter_norm = e_scale * norm + l_scale * z_norm
    for copy in ys:
        copy.wait_recv()
    before = jnp.zeros((share, dv), F32)
    for j in range(ny):
        before = y_scales[j][0] * before + y_scales[j][1] * y_in[j].astype(F32)
    for j in range(nz):
        e_buf[j] = (e_scales[j][0] * before + e_scales[j][1] * p_buf[j]).astype(BF16)
    es = []
    for d in order:
        peer = lax.rem(z + d, nz)
        copy = remote(e_buf.at[peer], e_in.at[z], e_ss.at[d], e_rs.at[d], {"z": peer})
        copy.start()
        es.append(copy)
    e_in[z] = e_buf[z]
    sends += es

    e_scale, l_scale, both_max = merge(chip_max, a_top, a_decay)
    both_norm = e_scale * enter_norm + l_scale * a_norm
    my_max, my_norm = jnp.where(first, chip_max, both_max), jnp.where(first, enter_norm, both_norm)
    write_info(finfo_out, jnp.where(first, both_norm, enter_norm), jnp.where(first, both_max, chip_max), a_decay, gate)
    finish = [remote(finfo_out, finfo_in, f_ss.at[0], f_rs.at[0], partner), remote(f_out, f_in, f_ss.at[1], f_rs.at[1], partner)]
    finish[0].start()
    for copy in es:
        copy.wait_recv()
    for j in range(nz):
        rows = pl.ds(j * share, share)
        entering = e_in[j].astype(F32)
        a_rows = jnp.where(first, own1[rows, :], pair_in[rows, :].astype(F32))
        both = e_scale * entering + l_scale * a_rows
        f_out[rows, :] = jnp.where(first, both, entering).astype(BF16)
        mine[rows, :] = jnp.where(first, entering, both).astype(BF16)
    finish[1].start()
    sends += finish

    def readout(s, carry, norm, top):
        for r in range(2):
            rows = pl.ds(r * half, half)
            q = q_buf[s, rows, :]
            carried = dot(q, carry[...])
            carried_den = jnp.sum(q.astype(F32) * norm, axis=1, keepdims=True)
            b_top = bmax_buf[s, rows, :]
            stabilizer = jnp.maximum(b_top, top)
            a, k = jnp.exp(b_top - stabilizer), jnp.exp(top - stabilizer)
            den = a * den_buf[s, rows, :] + k * carried_den
            inverse = 1.0 / jnp.maximum(jnp.abs(den), 1.0)
            hid[rows, s * dv : (s + 1) * dv] = ((a * inverse) * num_buf[s, rows, :] + (k * inverse) * carried).astype(BF16)

    readout(1, mine, my_norm, my_max)
    finish[0].wait_recv()
    other_norm, other_max, unused_decay, other_gate = read_info(finfo_in, 0)
    scale = 1.0 / (tokens * ny * nz * 2)
    kept, got = (gate * scale)[0, 0], (other_gate * scale)[0, 0]
    gate_ref[0] = jnp.where(first, kept, got)
    gate_ref[1] = jnp.where(first, got, kept)
    finish[1].wait_recv()
    readout(0, f_in, other_norm, other_max)

    step = 256
    quarter = tokens // 4

    def project(i, part, store):
        def body(n, carry):
            at = pl.ds(pl.multiple_of(n * step, step), step)
            out = dot(hid[part * half : (part + 1) * half, :], w_buf[i, :, at])
            store(part, at, out)
            return carry

        lax.fori_loop(0, cols // step, body, 0)

    def to(buf):
        def store(part, at, out):
            for r in range(2):
                buf[2 * part + r, :, at] = out[r * quarter : (r + 1) * quarter].astype(buf.dtype)

        return store

    def ship(src, dst, ss, rs, r, peer):
        copy = remote(src.at[r], dst.at[r], ss.at[r], rs.at[r], peer)
        copy.start()
        return copy

    for i in range(2):
        w_loads[i].wait()
    stage1 = [None] * 4
    for part in range(2):
        project(0, part, to(s1_out))
        for r in (2 * part, 2 * part + 1):
            stage1[r] = ship(s1_out, s1_in, s1_ss, s1_rs, r, left if part == 0 else right)
    direct = [None] * 4
    for i, part, peer in ((1, 1, left), (2, 0, right)):
        w_loads[2 * i].wait()
        w_loads[2 * i + 1].wait()
        project(i, part, to(dir_out))
        for r in (2 * part, 2 * part + 1):
            direct[r] = ship(dir_out, dir_in, dir_ss, dir_rs, r, peer)
    project(1, 0, to(rel_p))
    project(2, 1, to(rel_p))
    relay = [None] * 4
    for r in (0, 2, 1, 3):
        if r == 1:
            w_loads[6].wait()
            w_loads[7].wait()
            project(3, 0, to(own_p))
            project(3, 1, to(own_p))
        stage1[r].wait_recv()
        rel_out[r] = (rel_p[r] + s1_in[r].astype(F32)).astype(BF16)
        relay[r] = ship(rel_out, rel_in, rel_ss, rel_rs, r, left if r < 2 else right)
    sends += stage1 + direct + relay
    outs = []
    for r in (0, 2, 1, 3):
        direct[r].wait_recv()
        relay[r].wait_recv()
        out_buf[r] = (own_p[r] + dir_in[r].astype(F32) + rel_in[r].astype(F32)).astype(BF16)
        copy = pltpu.make_async_copy(out_buf.at[r], mixed_hbm.at[pl.ds(r * quarter, quarter), :], out_sem.at[r])
        copy.start()
        outs.append(copy)
    for copy in sends:
        copy.wait_send()
    for copy in outs:
        copy.wait()


def shards(queries, keys, values, forget_gate, input_gate, out_weight):
    tokens, heads = forget_gate.shape
    dk, dv = queries.shape[1] // heads, values.shape[1] // heads
    width = out_weight.shape[1]
    ny, nz, nx = (lax.axis_size(a) for a in ("y", "z", "x"))
    cols = width // nx
    share = dk // nz
    quarter = tokens // 4
    any_space = pl.BlockSpec(memory_space=pl.ANY)
    dma = pltpu.SemaphoreType.DMA
    info = lambda n: pltpu.VMEM((n, 1, INFO), F32)
    quad = lambda kind: pltpu.VMEM((4, quarter, cols), kind)
    mixed, gate_mean = pl.pallas_call(
        functools.partial(kernel, (ny, nz, nx)),
        out_shape=(jax.ShapeDtypeStruct((tokens, cols), BF16), jax.ShapeDtypeStruct((heads,), F32)),
        in_specs=[any_space] * 6,
        out_specs=(any_space, pl.BlockSpec(memory_space=pltpu.SMEM)),
        scratch_shapes=[
            pltpu.VMEM((2, tokens, dk), BF16),
            pltpu.VMEM((2, tokens, dk), BF16),
            pltpu.VMEM((2, tokens, dv), BF16),
            pltpu.VMEM((heads, tokens), F32),
            pltpu.VMEM((heads, tokens), F32),
            pltpu.VMEM((4, heads * dv, cols), BF16),
            pltpu.VMEM((2, dk, tokens), BF16),
            pltpu.VMEM((dk, dv), F32),
            pltpu.VMEM((dk, dv), BF16),
            pltpu.VMEM((dk, dv), BF16),
            info(1),
            info(1),
            pltpu.VMEM((nz, share, dv), BF16),
            pltpu.VMEM((nz, share, dv), BF16),
            info(1),
            info(nz),
            pltpu.VMEM((nz, share, dv), F32),
            pltpu.VMEM((share, dv), BF16),
            pltpu.VMEM((ny, share, dv), BF16),
            info(1),
            info(ny),
            pltpu.VMEM((nz, share, dv), BF16),
            pltpu.VMEM((nz, share, dv), BF16),
            pltpu.VMEM((dk, dv), BF16),
            pltpu.VMEM((dk, dv), BF16),
            info(1),
            info(1),
            pltpu.VMEM((dk, dv), BF16),
            pltpu.VMEM((2, tokens, dv), F32),
            pltpu.VMEM((2, tokens, 1), F32),
            pltpu.VMEM((2, tokens, 1), F32),
            pltpu.VMEM((tokens, heads * dv), BF16),
            quad(BF16), quad(BF16), quad(BF16), quad(BF16), quad(BF16), quad(BF16),
            quad(F32), quad(F32), quad(BF16),
            dma((8,)), dma((8,)), dma((4,)),
            dma((2,)), dma((2,)),
            dma((nz,)), dma((nz,)), dma((nz,)), dma((nz,)),
            dma((ny,)), dma((ny,)), dma((ny,)), dma((ny,)),
            dma((nz,)), dma((nz,)),
            dma((2,)), dma((2,)),
            dma((4,)), dma((4,)), dma((4,)), dma((4,)), dma((4,)), dma((4,)),
        ],
        compiler_params=pltpu.CompilerParams(
            collective_id=0, has_side_effects=True, vmem_limit_bytes=60 * 1024 * 1024
        ),
        name="mlstm_layer",
    )(queries, keys, values, forget_gate.T, input_gate.T, out_weight)
    return mixed, gate_mean


def solution(mesh):
    torus = Mesh(mesh.devices.reshape(4, 8, 2, mesh.shape["head"]), ("y", "z", "c", "x"))
    both = P(SEQ, "x")
    return jax.shard_map(
        shards,
        mesh=torus,
        in_specs=(both, both, both, both, both, P("x", None)),
        out_specs=(P(SEQ, "x"), P("x")),
        check_vma=False,
    )
```

```python
import functools

import jax
import jax.numpy as jnp
from jax import lax
from jax.experimental import pallas as pl
from jax.experimental.pallas import tpu as pltpu
from jax.sharding import Mesh
from jax.sharding import PartitionSpec as P

MESH = pl.DeviceIdType.MESH
SEQ = ("y", "z", "c")
F32 = jnp.float32
BF16 = jnp.bfloat16
LOW = -1e30
INFO = 640


def dot(a, b):
    return jnp.dot(a, b, preferred_element_type=F32)


def merge(e_max, l_max, l_decay):
    top = jnp.maximum(l_decay + e_max, l_max)
    return jnp.exp(l_decay + e_max - top), jnp.exp(l_max - top), top


def three_rows(row, first):
    hi = row.astype(BF16).astype(F32)
    mid = (row - hi).astype(BF16).astype(F32)
    low = row - hi - mid
    return jnp.where(first == 0, hi, jnp.where(first == 1, mid, jnp.where(first == 2, low, 0.0))).astype(BF16)


def read_info(ref, j):
    row = ref[j]
    return row[:, :256], row[:, 256:257], row[:, 384:385], row[:, 512:513]


def write_info(ref, norm, top, decay, gate):
    ref[0, :, 0:256] = norm
    ref[0, :, 256:384] = jnp.broadcast_to(top, (1, 128))
    ref[0, :, 384:512] = jnp.broadcast_to(decay, (1, 128))
    ref[0, :, 512:640] = jnp.broadcast_to(gate, (1, 128))


def kernel(
    sizes,
    q_hbm, k_hbm, v_hbm, fg_hbm, ig_hbm, w_hbm,
    mixed_ref, gate_ref,
    q_buf, k_buf, v_buf, fg_buf, ig_buf, w_buf, kt_buf,
    own1, pair_out, pair_in, pinfo_out, pinfo_in,
    t_buf, t_in, tinfo_out, tinfo,
    p_buf, y_out, y_in, yinfo_out, yinfo,
    e_buf, e_in, f_out, f_in, finfo_out, finfo_in, mine,
    num_buf, bmax_buf, den_buf, hid,
    s1_out, s1_in, dir_out, dir_in, rel_out, rel_in, own_p,
    load_sem, w_sem,
    pair_ss, pair_rs, z_ss, z_rs, zi_ss, zi_rs, y_ss, y_rs, yi_ss, yi_rs, e_ss, e_rs, f_ss, f_rs, fi_ss, fi_rs,
    s1_ss, s1_rs, dir_ss, dir_rs, rel_ss, rel_rs,
):
    ny, nz, nx = sizes
    y, z, c, x = (lax.axis_index(a) for a in ("y", "z", "c", "x"))
    tokens = q_buf.shape[1]
    dk, dv = q_buf.shape[2], v_buf.shape[2]
    half = tokens // 2
    cols = w_buf.shape[2]
    share = dk // nz
    chunks, wide, step = t_buf.shape[0], t_buf.shape[3], own_p.shape[2]
    first = c == 0
    heads = (1 - c, c)

    loads = []

    def load(src, dst):
        copy = pltpu.make_async_copy(src, dst, load_sem.at[len(loads)])
        copy.start()
        loads.append(copy)

    load(fg_hbm, fg_buf)
    load(ig_hbm, ig_buf)
    for s in range(2):
        load(k_hbm.at[:, pl.ds(pl.multiple_of(heads[s] * dk, 128), dk)], k_buf.at[s])
        load(v_hbm.at[:, pl.ds(pl.multiple_of(heads[s] * dv, 128), dv)], v_buf.at[s])
    for s in range(2):
        load(q_hbm.at[:, pl.ds(pl.multiple_of(heads[s] * dk, 128), dk)], q_buf.at[s])

    barrier = pltpu.get_barrier_semaphore()
    peers = [{"c": 1 - c}]
    peers += [{"z": lax.rem(z + d, nz)} for d in range(1, nz)]
    peers += [{"y": lax.rem(y + d, ny)} for d in range(1, ny)]
    left, right = {"x": lax.rem(x + nx - 1, nx)}, {"x": lax.rem(x + 1, nx)}
    peers += [left, right]
    for peer in peers:
        pl.semaphore_signal(barrier, inc=1, device_id=peer, device_id_type=MESH)

    targets = (lax.rem(x + 2, nx), lax.rem(x + nx - 1, nx), lax.rem(x + 1, nx), x)
    w_loads = []
    for i in range(4):
        for s in range(2):
            copy = pltpu.make_async_copy(
                w_hbm.at[pl.ds(pl.multiple_of(heads[s] * dv, 128), dv), pl.ds(pl.multiple_of(targets[i] * cols, 128), cols)],
                w_buf.at[i, pl.ds(s * dv, dv), :],
                w_sem.at[2 * i + s],
            )
            copy.start()
            w_loads.append(copy)

    loads[0].wait()
    loads[1].wait()
    fg, ig = fg_buf[...], ig_buf[...]
    lf = jnp.minimum(fg, 0.0) - jnp.log1p(jnp.exp(-jnp.abs(fg)))
    lf_rows = (jnp.where(first, lf[1:2], lf[0:1]), jnp.where(first, lf[0:1], lf[1:2]))
    ig_rows = (jnp.where(first, ig[1:2], ig[0:1]), jnp.where(first, ig[0:1], ig[1:2]))
    sub = lax.broadcasted_iota(jnp.int32, (8, tokens), 0)
    upper = (
        lax.broadcasted_iota(jnp.int32, (tokens, tokens), 0) <= lax.broadcasted_iota(jnp.int32, (tokens, tokens), 1)
    ).astype(F32).astype(BF16)
    stacked = jnp.where(
        sub < 4,
        three_rows(jnp.broadcast_to(lf_rows[0], (8, tokens)), sub).astype(F32),
        three_rows(jnp.broadcast_to(lf_rows[1], (8, tokens)), sub - 4).astype(F32),
    ).astype(BF16)
    cums = dot(stacked, upper)
    b_rows, decays, tops, weights = [], [], [], []
    for s in range(2):
        cum = jnp.sum(cums[4 * s : 4 * s + 4], axis=0, keepdims=True)
        b = ig_rows[s] - cum
        decay = cum[:, tokens - 1 : tokens]
        b_top = jnp.max(b, axis=1, keepdims=True)
        b_rows.append(b)
        decays.append(decay)
        tops.append(decay + b_top)
        weights.append(jnp.exp(b - b_top) * (dk**-0.5))
    gates = [jnp.sum(ig_rows[s], axis=1, keepdims=True) for s in range(2)]

    def own_state(s):
        kt = k_buf[s].T
        kt_buf[s] = kt
        wkt = (kt.astype(F32) * weights[s]).astype(BF16)
        matrix = dot(wkt, v_buf[s])
        norm = jnp.sum(dot(three_rows(jnp.broadcast_to(weights[s], (8, tokens)), sub), k_buf[s]), axis=0, keepdims=True)
        return matrix, norm

    def remote(src, dst, ss, rs, peer):
        return pltpu.make_async_remote_copy(
            src_ref=src, dst_ref=dst, send_sem=ss, recv_sem=rs, device_id=peer, device_id_type=MESH
        )

    sends = []

    loads[2].wait()
    loads[3].wait()
    matrix0, norm0 = own_state(0)
    pair_out[...] = matrix0.astype(BF16)
    write_info(pinfo_out, norm0, tops[0], decays[0], gates[0])
    pl.semaphore_wait(barrier, len(peers))
    partner = {"c": 1 - c}
    pair = [
        remote(pinfo_out, pinfo_in, pair_ss.at[0], pair_rs.at[0], partner),
        remote(pair_out, pair_in, pair_ss.at[1], pair_rs.at[1], partner),
    ]
    for copy in pair:
        copy.start()
    sends += pair

    loads[4].wait()
    loads[5].wait()
    matrix1, norm1 = own_state(1)
    own1[...] = matrix1

    pair[0].wait_recv()
    in_norm, in_top, in_decay, in_gate = read_info(pinfo_in, 0)
    a_top, a_norm = jnp.where(first, tops[1], in_top), jnp.where(first, norm1, in_norm)
    a_decay = jnp.where(first, decays[1], in_decay)
    l_top, l_norm = jnp.where(first, in_top, tops[1]), jnp.where(first, in_norm, norm1)
    l_decay = jnp.where(first, in_decay, decays[1])
    e_scale, l_scale, chip_top = merge(a_top, l_top, l_decay)
    chip_norm = e_scale * a_norm + l_scale * l_norm
    write_info(tinfo_out, chip_norm, chip_top, a_decay + l_decay, gates[1] + in_gate)
    zi = []
    order = sorted(range(1, nz), key=lambda d: -min(d, nz - d))
    for d in order:
        copy = remote(tinfo_out.at[0], tinfo.at[z], zi_ss.at[d], zi_rs.at[d], {"z": lax.rem(z + d, nz)})
        copy.start()
        zi.append(copy)
    tinfo[z] = tinfo_out[0]
    own_scale, in_scale = jnp.where(first, e_scale, l_scale), jnp.where(first, l_scale, e_scale)
    pair[1].wait_recv()
    zs = []
    for h in range(chunks):
        at = pl.ds(h * wide, wide)
        for j in range(nz):
            rows = pl.ds(j * share, share)
            t_buf[h, j] = (own_scale * own1[rows, at] + in_scale * pair_in[rows, at].astype(F32)).astype(BF16)
        zs.append([])
        for d in order:
            peer = lax.rem(z + d, nz)
            copy = remote(t_buf.at[h, peer], t_in.at[h, z], z_ss.at[h, d], z_rs.at[h, d], {"z": peer})
            copy.start()
            zs[h].append(copy)
        t_in[h, z] = t_buf[h, z]
        sends += zs[h]
    sends += zi

    loads[6].wait()
    loads[7].wait()

    def intra(s):
        for r in range(2):
            rows = pl.ds(r * half, half)
            span = half * (r + 1)
            scores = dot(q_buf[s, rows, :], kt_buf[s, :, :span]) * (dk**-0.5)
            t_index = lax.broadcasted_iota(jnp.int32, (half, span), 0) + r * half
            s_index = lax.broadcasted_iota(jnp.int32, (half, span), 1)
            logs = jnp.where(s_index <= t_index, jnp.broadcast_to(b_rows[s][:, :span], (half, span)), -jnp.inf)
            top = jnp.max(logs, axis=1, keepdims=True)
            weighted = jnp.exp(logs - top) * scores
            bmax_buf[s, rows, :] = top
            den_buf[s, rows, :] = jnp.sum(weighted, axis=1, keepdims=True)
            num_buf[s, rows, :] = dot(weighted.astype(BF16), v_buf[s, :span, :])

    intra(1)
    intra(0)

    for copy in zi:
        copy.wait_recv()
    top, decay, norm, gate = jnp.full((1, 1), LOW, F32), jnp.zeros((1, 1), F32), jnp.zeros((1, dk), F32), jnp.zeros((1, 1), F32)
    z_norm, z_top, z_decay = norm, top, decay
    z_tops, z_decays, scales = [], [], []
    for j in range(nz):
        z_tops.append(top)
        z_decays.append(decay)
        here = j == z
        z_norm, z_top, z_decay = jnp.where(here, norm, z_norm), jnp.where(here, top, z_top), jnp.where(here, decay, z_decay)
        j_norm, j_top, j_decay, j_gate = read_info(tinfo, j)
        e_scale, l_scale, top = merge(top, j_top, j_decay)
        norm = e_scale * norm + l_scale * j_norm
        decay = decay + j_decay
        gate = gate + j_gate
        scales.append((e_scale, l_scale))
    write_info(yinfo_out, norm, top, decay, gate)
    yi = []
    y_order = sorted(range(1, ny), key=lambda d: -min(d, ny - d))
    for d in y_order:
        copy = remote(yinfo_out.at[0], yinfo.at[y], yi_ss.at[d], yi_rs.at[d], {"y": lax.rem(y + d, ny)})
        copy.start()
        yi.append(copy)
    yinfo[y] = yinfo_out[0]
    ys = []
    for h in range(chunks):
        for copy in zs[h]:
            copy.wait_recv()
        running = jnp.zeros((share, wide), F32)
        for j in range(nz):
            p_buf[h, j] = running
            running = scales[j][0] * running + scales[j][1] * t_in[h, j].astype(F32)
        y_out[h] = running.astype(BF16)
        ys.append([])
        for d in y_order:
            copy = remote(y_out.at[h], y_in.at[h, y], y_ss.at[h, d], y_rs.at[h, d], {"y": lax.rem(y + d, ny)})
            copy.start()
            ys[h].append(copy)
        y_in[h, y] = y_out[h]
        sends += ys[h]
    sends += yi

    for copy in yi:
        copy.wait_recv()
    top, decay, norm, gate = jnp.full((1, 1), LOW, F32), jnp.zeros((1, 1), F32), jnp.zeros((1, dk), F32), jnp.zeros((1, 1), F32)
    y_scales = []
    for j in range(ny):
        j_norm, j_top, j_decay, j_gate = read_info(yinfo, j)
        passed = j < y
        e_scale, l_scale, next_top = merge(top, j_top, j_decay)
        norm = jnp.where(passed, e_scale * norm + l_scale * j_norm, norm)
        top = jnp.where(passed, next_top, top)
        gate = gate + j_gate
        y_scales.append((jnp.where(passed, e_scale, 1.0), jnp.where(passed, l_scale, 0.0)))
    e_scales = [merge(top, z_tops[j], z_decays[j]) for j in range(nz)]
    e_scale, l_scale, chip_max = merge(top, z_top, z_decay)
    enter_norm = e_scale * norm + l_scale * z_norm

    e_scale, l_scale, both_max = merge(chip_max, a_top, a_decay)
    both_norm = e_scale * enter_norm + l_scale * a_norm
    my_max, my_norm = jnp.where(first, chip_max, both_max), jnp.where(first, enter_norm, both_norm)
    write_info(finfo_out, jnp.where(first, both_norm, enter_norm), jnp.where(first, both_max, chip_max), a_decay, gate)
    ahead = remote(finfo_out, finfo_in, fi_ss.at[0], fi_rs.at[0], partner)
    ahead.start()
    sends.append(ahead)

    es = []
    for h in range(chunks):
        for copy in ys[h]:
            copy.wait_recv()
        before = jnp.zeros((share, wide), F32)
        for j in range(ny):
            before = y_scales[j][0] * before + y_scales[j][1] * y_in[h, j].astype(F32)
        for j in range(nz):
            e_buf[h, j] = (e_scales[j][0] * before + e_scales[j][1] * p_buf[h, j]).astype(BF16)
        es.append([])
        for d in order:
            peer = lax.rem(z + d, nz)
            copy = remote(e_buf.at[h, peer], e_in.at[h, z], e_ss.at[h, d], e_rs.at[h, d], {"z": peer})
            copy.start()
            es[h].append(copy)
        e_in[h, z] = e_buf[h, z]
        sends += es[h]

    def factors(s, norm, top):
        for r in range(2):
            rows = pl.ds(r * half, half)
            carried_den = jnp.sum(q_buf[s, rows, :].astype(F32) * norm, axis=1, keepdims=True)
            b_top = bmax_buf[s, rows, :]
            stabilizer = jnp.maximum(b_top, top)
            a, k = jnp.exp(b_top - stabilizer), jnp.exp(top - stabilizer)
            den = a * den_buf[s, rows, :] + k * carried_den
            inverse = 1.0 / jnp.maximum(jnp.abs(den), 1.0)
            bmax_buf[s, rows, :] = a * inverse
            den_buf[s, rows, :] = k * inverse

    factors(1, my_norm, my_max)
    ahead.wait_recv()
    other_norm, other_max, unused_decay, other_gate = read_info(finfo_in, 0)
    scale = 1.0 / (tokens * ny * nz * 2)
    lane = lax.broadcasted_iota(jnp.int32, (1, 2), 1)
    gate_ref[...] = jnp.where(lane == c, gate, other_gate) * scale
    factors(0, other_norm, other_max)

    def readout(s, h, carry):
        for r in range(2):
            rows = pl.ds(r * half, half)
            carried = dot(q_buf[s, rows, :], carry)
            own = num_buf[s, rows, h * wide : (h + 1) * wide]
            at = s * dv + h * wide
            hid[rows, at : at + wide] = (bmax_buf[s, rows, :] * own + den_buf[s, rows, :] * carried).astype(BF16)

    finish = []
    for h in range(chunks):
        for copy in es[h]:
            copy.wait_recv()
        for j in range(nz):
            rows = pl.ds(j * share, share)
            entering = e_in[h, j].astype(F32)
            a_rows = jnp.where(first, own1[rows, h * wide : (h + 1) * wide], pair_in[rows, h * wide : (h + 1) * wide].astype(F32))
            both = e_scale * entering + l_scale * a_rows
            f_out[h, rows, :] = jnp.where(first, both, entering).astype(BF16)
            mine[h, rows, :] = jnp.where(first, entering, both).astype(BF16)
        copy = remote(f_out.at[h], f_in.at[h], f_ss.at[h], f_rs.at[h], partner)
        copy.start()
        finish.append(copy)
        readout(1, h, mine[h])
    sends += finish
    for h in range(chunks):
        finish[h].wait_recv()
        readout(0, h, f_in[h])

    def piece(i, part, n):
        return dot(hid[part * half : (part + 1) * half, :], w_buf[i, :, n * step : (n + 1) * step])

    def ship(src, dst, ss, rs, r, peer):
        copy = remote(src.at[r], dst.at[r], ss.at[r], rs.at[r], peer)
        copy.start()
        return copy

    def loaded(i):
        w_loads[2 * i].wait()
        w_loads[2 * i + 1].wait()

    parts = cols // step
    towards = (left, right)
    stage1, direct, relay = [], [], []
    loaded(0)
    for n in range(parts):
        for part in range(2):
            r = 2 * n + part
            s1_out[r] = piece(0, part, n).astype(BF16)
            stage1.append(ship(s1_out, s1_in, s1_ss, s1_rs, r, towards[part]))
    loaded(1)
    loaded(2)
    for n in range(parts):
        for part in range(2):
            r = 2 * n + part
            dir_out[r] = piece(2 - part, part, n).astype(BF16)
            direct.append(ship(dir_out, dir_in, dir_ss, dir_rs, r, towards[1 - part]))
    for n in range(parts):
        for part in range(2):
            r = 2 * n + part
            partial = piece(1 + part, part, n)
            stage1[r].wait_recv()
            rel_out[r] = (partial + s1_in[r].astype(F32)).astype(BF16)
            relay.append(ship(rel_out, rel_in, rel_ss, rel_rs, r, towards[part]))
    loaded(3)
    for n in range(parts):
        for part in range(2):
            own_p[2 * n + part] = piece(3, part, n)
    sends += stage1 + direct + relay
    for n in range(parts):
        for part in range(2):
            r = 2 * n + part
            direct[r].wait_recv()
            partial = own_p[r] + dir_in[r].astype(F32)
            relay[r].wait_recv()
            mixed_ref[part * half : (part + 1) * half, n * step : (n + 1) * step] = (partial + rel_in[r].astype(F32)).astype(BF16)
    for copy in sends:
        copy.wait_send()


def shards(queries, keys, values, forget_gate, input_gate, out_weight):
    tokens, heads = forget_gate.shape
    dk, dv = queries.shape[1] // heads, values.shape[1] // heads
    width = out_weight.shape[1]
    ny, nz, nx = (lax.axis_size(a) for a in ("y", "z", "x"))
    cols = width // nx
    share = dk // nz
    chunks, step = 4, 256
    wide, count = dv // chunks, 2 * cols // step
    any_space = pl.BlockSpec(memory_space=pltpu.HBM)
    dma = pltpu.SemaphoreType.DMA
    info = lambda n: pltpu.VMEM((n, 1, INFO), F32)
    pieces = lambda kind: pltpu.VMEM((count, tokens // 2, step), kind)
    mixed, gate_mean = pl.pallas_call(
        functools.partial(kernel, (ny, nz, nx)),
        out_shape=(pltpu.VMEM((tokens, cols), BF16), pltpu.VMEM((1, heads), F32)),
        in_specs=[any_space] * 6,
        out_specs=(pl.BlockSpec(memory_space=pltpu.VMEM), pl.BlockSpec(memory_space=pltpu.VMEM)),
        scratch_shapes=[
            pltpu.VMEM((2, tokens, dk), BF16),
            pltpu.VMEM((2, tokens, dk), BF16),
            pltpu.VMEM((2, tokens, dv), BF16),
            pltpu.VMEM((heads, tokens), F32),
            pltpu.VMEM((heads, tokens), F32),
            pltpu.VMEM((4, heads * dv, cols), BF16),
            pltpu.VMEM((2, dk, tokens), BF16),
            pltpu.VMEM((dk, dv), F32),
            pltpu.VMEM((dk, dv), BF16),
            pltpu.VMEM((dk, dv), BF16),
            info(1),
            info(1),
            pltpu.VMEM((chunks, nz, share, wide), BF16),
            pltpu.VMEM((chunks, nz, share, wide), BF16),
            info(1),
            info(nz),
            pltpu.VMEM((chunks, nz, share, wide), F32),
            pltpu.VMEM((chunks, share, wide), BF16),
            pltpu.VMEM((chunks, ny, share, wide), BF16),
            info(1),
            info(ny),
            pltpu.VMEM((chunks, nz, share, wide), BF16),
            pltpu.VMEM((chunks, nz, share, wide), BF16),
            pltpu.VMEM((chunks, dk, wide), BF16),
            pltpu.VMEM((chunks, dk, wide), BF16),
            info(1),
            info(1),
            pltpu.VMEM((chunks, dk, wide), BF16),
            pltpu.VMEM((2, tokens, dv), F32),
            pltpu.VMEM((2, tokens, 1), F32),
            pltpu.VMEM((2, tokens, 1), F32),
            pltpu.VMEM((tokens, heads * dv), BF16),
            pieces(BF16), pieces(BF16), pieces(BF16), pieces(BF16), pieces(BF16), pieces(BF16), pieces(F32),
            dma((8,)), dma((8,)),
            dma((2,)), dma((2,)),
            dma((chunks, nz)), dma((chunks, nz)), dma((nz,)), dma((nz,)),
            dma((chunks, ny)), dma((chunks, ny)), dma((ny,)), dma((ny,)),
            dma((chunks, nz)), dma((chunks, nz)),
            dma((chunks,)), dma((chunks,)), dma((1,)), dma((1,)),
            dma((count,)), dma((count,)), dma((count,)), dma((count,)), dma((count,)), dma((count,)),
        ],
        compiler_params=pltpu.CompilerParams(
            collective_id=0, has_side_effects=True, vmem_limit_bytes=65000000
        ),
        name="mlstm_layer",
    )(queries, keys, values, forget_gate.T, input_gate.T, out_weight)
    return mixed, gate_mean.reshape(heads)


def solution(mesh):
    torus = Mesh(mesh.devices.reshape(4, 8, 2, mesh.shape["head"]), ("y", "z", "c", "x"))
    both = P(SEQ, "x")
    return jax.shard_map(
        shards,
        mesh=torus,
        in_specs=(both, both, both, both, both, P("x", None)),
        out_specs=(P(SEQ, "x"), P("x")),
        check_vma=False,
    )
```

```python
import functools

import jax
import jax.numpy as jnp
from jax import lax
from jax.experimental import pallas as pl
from jax.experimental.pallas import tpu as pltpu
from jax.sharding import Mesh
from jax.sharding import PartitionSpec as P

MESH = pl.DeviceIdType.MESH
SEQ = ("y", "z", "c")
F32 = jnp.float32
BF16 = jnp.bfloat16
LOW = -1e30
INFO = 640


def dot(a, b):
    return jnp.dot(a, b, preferred_element_type=F32)


def merge(e_max, l_max, l_decay):
    top = jnp.maximum(l_decay + e_max, l_max)
    return jnp.exp(l_decay + e_max - top), jnp.exp(l_max - top), top


def three_rows(row, first):
    hi = row.astype(BF16).astype(F32)
    mid = (row - hi).astype(BF16).astype(F32)
    low = row - hi - mid
    return jnp.where(first == 0, hi, jnp.where(first == 1, mid, jnp.where(first == 2, low, 0.0))).astype(BF16)


def read_info(ref, j):
    row = ref[j]
    return row[:, :256], row[:, 256:257], row[:, 384:385], row[:, 512:513]


def write_info(ref, norm, top, decay, gate):
    ref[0, :, 0:256] = norm
    ref[0, :, 256:384] = jnp.broadcast_to(top, (1, 128))
    ref[0, :, 384:512] = jnp.broadcast_to(decay, (1, 128))
    ref[0, :, 512:640] = jnp.broadcast_to(gate, (1, 128))


def kernel(
    sizes,
    q_hbm, k_hbm, v_hbm, fg_hbm, ig_hbm, w_hbm,
    mixed_ref, gate_ref,
    q_buf, k_buf, v_buf, fg_buf, ig_buf, w_buf, kt_buf,
    own1, pair_out, pair_in, pinfo_out, pinfo_in,
    t_buf, t_in, tinfo_out, tinfo,
    p_buf, y_out, y_in, yinfo_out, yinfo,
    e_buf, e_in, f_out, f_in, finfo_out, finfo_in, mine,
    num_buf, bmax_buf, den_buf, hid,
    ag_in, acc,
    load_sem, w_sem,
    pair_ss, pair_rs, z_ss, z_rs, zi_ss, zi_rs, y_ss, y_rs, yi_ss, yi_rs, e_ss, e_rs, f_ss, f_rs, fi_ss, fi_rs,
    wx_ss, wx_rs, wy_ss, wy_rs, wf_ss, wf_rs, wp_ss, wp_rs, ag_ss, ag_rs, af_ss, af_rs,
):
    ny, nz, nx = sizes
    y, z, c, x = (lax.axis_index(a) for a in ("y", "z", "c", "x"))
    tokens = q_buf.shape[1]
    dk, dv = q_buf.shape[2], v_buf.shape[2]
    half = tokens // 2
    cols = w_buf.shape[2]
    slab = w_buf.shape[1] // (2 * ny)
    share = dk // nz
    chunks, wide, step = t_buf.shape[0], t_buf.shape[3], acc.shape[2]
    first = c == 0
    heads = (1 - c, c)

    loads = []

    def load(src, dst):
        copy = pltpu.make_async_copy(src, dst, load_sem.at[len(loads)])
        copy.start()
        loads.append(copy)

    load(fg_hbm, fg_buf)
    load(ig_hbm, ig_buf)
    for s in range(2):
        load(k_hbm.at[:, pl.ds(pl.multiple_of(heads[s] * dk, 128), dk)], k_buf.at[s])
        load(v_hbm.at[:, pl.ds(pl.multiple_of(heads[s] * dv, 128), dv)], v_buf.at[s])
    for s in range(2):
        load(q_hbm.at[:, pl.ds(pl.multiple_of(heads[s] * dk, 128), dk)], q_buf.at[s])

    barrier = pltpu.get_barrier_semaphore()
    peers = [{"c": 1 - c}]
    peers += [{"z": lax.rem(z + d, nz)} for d in range(1, nz)]
    peers += [{"y": lax.rem(y + d, ny)} for d in range(1, ny)]
    left, right = {"x": lax.rem(x + nx - 1, nx)}, {"x": lax.rem(x + 1, nx)}
    far = {"x": lax.rem(x + 2, nx)}
    peers += [left, right, far]
    for peer in peers:
        pl.semaphore_signal(barrier, inc=1, device_id=peer, device_id_type=MESH)

    loads[0].wait()
    loads[1].wait()
    fg, ig = fg_buf[...], ig_buf[...]
    lf = jnp.minimum(fg, 0.0) - jnp.log1p(jnp.exp(-jnp.abs(fg)))
    lf_rows = (jnp.where(first, lf[1:2], lf[0:1]), jnp.where(first, lf[0:1], lf[1:2]))
    ig_rows = (jnp.where(first, ig[1:2], ig[0:1]), jnp.where(first, ig[0:1], ig[1:2]))
    sub = lax.broadcasted_iota(jnp.int32, (8, tokens), 0)
    upper = (
        lax.broadcasted_iota(jnp.int32, (tokens, tokens), 0) <= lax.broadcasted_iota(jnp.int32, (tokens, tokens), 1)
    ).astype(F32).astype(BF16)
    stacked = jnp.where(
        sub < 4,
        three_rows(jnp.broadcast_to(lf_rows[0], (8, tokens)), sub).astype(F32),
        three_rows(jnp.broadcast_to(lf_rows[1], (8, tokens)), sub - 4).astype(F32),
    ).astype(BF16)
    cums = dot(stacked, upper)
    b_rows, decays, tops, weights = [], [], [], []
    for s in range(2):
        cum = jnp.sum(cums[4 * s : 4 * s + 4], axis=0, keepdims=True)
        b = ig_rows[s] - cum
        decay = cum[:, tokens - 1 : tokens]
        b_top = jnp.max(b, axis=1, keepdims=True)
        b_rows.append(b)
        decays.append(decay)
        tops.append(decay + b_top)
        weights.append(jnp.exp(b - b_top) * (dk**-0.5))
    gates = [jnp.sum(ig_rows[s], axis=1, keepdims=True) for s in range(2)]

    def own_state(s):
        kt = k_buf[s].T
        kt_buf[s] = kt
        wkt = (kt.astype(F32) * weights[s]).astype(BF16)
        matrix = dot(wkt, v_buf[s])
        norm = jnp.sum(dot(three_rows(jnp.broadcast_to(weights[s], (8, tokens)), sub), k_buf[s]), axis=0, keepdims=True)
        return matrix, norm

    def remote(src, dst, ss, rs, peer):
        return pltpu.make_async_remote_copy(
            src_ref=src, dst_ref=dst, send_sem=ss, recv_sem=rs, device_id=peer, device_id_type=MESH
        )

    sends = []

    loads[2].wait()
    loads[3].wait()
    matrix0, norm0 = own_state(0)
    pair_out[...] = matrix0.astype(BF16)
    write_info(pinfo_out, norm0, tops[0], decays[0], gates[0])
    pl.semaphore_wait(barrier, len(peers))
    partner = {"c": 1 - c}
    pair = [
        remote(pinfo_out, pinfo_in, pair_ss.at[0], pair_rs.at[0], partner),
        remote(pair_out, pair_in, pair_ss.at[1], pair_rs.at[1], partner),
    ]
    for copy in pair:
        copy.start()
    sends += pair

    def slab_of(y_index, c_index):
        return pl.multiple_of((y_index * 2 + c_index) * slab, slab)

    mine_rows = pl.ds(slab_of(y, c), slab)
    wx = []
    for i, peer in ((0, right), (1, left), (2, far)):
        copy = remote(
            w_hbm.at[mine_rows, pl.ds(pl.multiple_of(peer["x"] * cols, 128), cols)], w_buf.at[i, mine_rows, :], wx_ss.at[i], wx_rs.at[i], peer
        )
        copy.start()
        wx.append(copy)
    sends += wx
    w_own = pltpu.make_async_copy(w_hbm.at[:, pl.ds(pl.multiple_of(x * cols, 128), cols)], w_buf.at[3], w_sem.at[0])

    loads[4].wait()
    loads[5].wait()
    matrix1, norm1 = own_state(1)
    own1[...] = matrix1

    pair[0].wait_recv()
    in_norm, in_top, in_decay, in_gate = read_info(pinfo_in, 0)
    a_top, a_norm = jnp.where(first, tops[1], in_top), jnp.where(first, norm1, in_norm)
    a_decay = jnp.where(first, decays[1], in_decay)
    l_top, l_norm = jnp.where(first, in_top, tops[1]), jnp.where(first, in_norm, norm1)
    l_decay = jnp.where(first, in_decay, decays[1])
    e_scale, l_scale, chip_top = merge(a_top, l_top, l_decay)
    chip_norm = e_scale * a_norm + l_scale * l_norm
    write_info(tinfo_out, chip_norm, chip_top, a_decay + l_decay, gates[1] + in_gate)
    zi = []
    order = sorted(range(1, nz), key=lambda d: -min(d, nz - d))
    for d in order:
        copy = remote(tinfo_out.at[0], tinfo.at[z], zi_ss.at[d], zi_rs.at[d], {"z": lax.rem(z + d, nz)})
        copy.start()
        zi.append(copy)
    tinfo[z] = tinfo_out[0]
    own_scale, in_scale = jnp.where(first, e_scale, l_scale), jnp.where(first, l_scale, e_scale)
    pair[1].wait_recv()
    zs = []
    for h in range(chunks):
        at = pl.ds(h * wide, wide)
        for j in range(nz):
            rows = pl.ds(j * share, share)
            t_buf[h, j] = (own_scale * own1[rows, at] + in_scale * pair_in[rows, at].astype(F32)).astype(BF16)
        zs.append([])
        for d in order:
            peer = lax.rem(z + d, nz)
            copy = remote(t_buf.at[h, peer], t_in.at[h, z], z_ss.at[h, d], z_rs.at[h, d], {"z": peer})
            copy.start()
            zs[h].append(copy)
        t_in[h, z] = t_buf[h, z]
        sends += zs[h]
    sends += zi

    w_own.start()

    loads[6].wait()
    loads[7].wait()

    def intra(s):
        for r in range(2):
            rows = pl.ds(r * half, half)
            span = half * (r + 1)
            scores = dot(q_buf[s, rows, :], kt_buf[s, :, :span]) * (dk**-0.5)
            t_index = lax.broadcasted_iota(jnp.int32, (half, span), 0) + r * half
            s_index = lax.broadcasted_iota(jnp.int32, (half, span), 1)
            logs = jnp.where(s_index <= t_index, jnp.broadcast_to(b_rows[s][:, :span], (half, span)), -jnp.inf)
            top = jnp.max(logs, axis=1, keepdims=True)
            weighted = jnp.exp(logs - top) * scores
            bmax_buf[s, rows, :] = top
            den_buf[s, rows, :] = jnp.sum(weighted, axis=1, keepdims=True)
            num_buf[s, rows, :] = dot(weighted.astype(BF16), v_buf[s, :span, :])

    intra(1)
    intra(0)

    for copy in zi:
        copy.wait_recv()
    top, decay, norm, gate = jnp.full((1, 1), LOW, F32), jnp.zeros((1, 1), F32), jnp.zeros((1, dk), F32), jnp.zeros((1, 1), F32)
    z_norm, z_top, z_decay = norm, top, decay
    z_tops, z_decays, scales = [], [], []
    for j in range(nz):
        z_tops.append(top)
        z_decays.append(decay)
        here = j == z
        z_norm, z_top, z_decay = jnp.where(here, norm, z_norm), jnp.where(here, top, z_top), jnp.where(here, decay, z_decay)
        j_norm, j_top, j_decay, j_gate = read_info(tinfo, j)
        e_scale, l_scale, top = merge(top, j_top, j_decay)
        norm = e_scale * norm + l_scale * j_norm
        decay = decay + j_decay
        gate = gate + j_gate
        scales.append((e_scale, l_scale))
    write_info(yinfo_out, norm, top, decay, gate)
    yi = []
    y_order = sorted(range(1, ny), key=lambda d: -min(d, ny - d))
    for d in y_order:
        copy = remote(yinfo_out.at[0], yinfo.at[y], yi_ss.at[d], yi_rs.at[d], {"y": lax.rem(y + d, ny)})
        copy.start()
        yi.append(copy)
    yinfo[y] = yinfo_out[0]
    ys = []
    for h in range(chunks):
        for copy in zs[h]:
            copy.wait_recv()
        running = jnp.zeros((share, wide), F32)
        for j in range(nz):
            p_buf[h, j] = running
            running = scales[j][0] * running + scales[j][1] * t_in[h, j].astype(F32)
        y_out[h] = running.astype(BF16)
        ys.append([])
        for d in y_order:
            copy = remote(y_out.at[h], y_in.at[h, y], y_ss.at[h, d], y_rs.at[h, d], {"y": lax.rem(y + d, ny)})
            copy.start()
            ys[h].append(copy)
        y_in[h, y] = y_out[h]
        sends += ys[h]
    sends += yi

    for copy in yi:
        copy.wait_recv()
    top, decay, norm, gate = jnp.full((1, 1), LOW, F32), jnp.zeros((1, 1), F32), jnp.zeros((1, dk), F32), jnp.zeros((1, 1), F32)
    y_scales = []
    for j in range(ny):
        j_norm, j_top, j_decay, j_gate = read_info(yinfo, j)
        passed = j < y
        e_scale, l_scale, next_top = merge(top, j_top, j_decay)
        norm = jnp.where(passed, e_scale * norm + l_scale * j_norm, norm)
        top = jnp.where(passed, next_top, top)
        gate = gate + j_gate
        y_scales.append((jnp.where(passed, e_scale, 1.0), jnp.where(passed, l_scale, 0.0)))
    e_scales = [merge(top, z_tops[j], z_decays[j]) for j in range(nz)]
    e_scale, l_scale, chip_max = merge(top, z_top, z_decay)
    enter_norm = e_scale * norm + l_scale * z_norm

    e_scale, l_scale, both_max = merge(chip_max, a_top, a_decay)
    both_norm = e_scale * enter_norm + l_scale * a_norm
    my_max, my_norm = jnp.where(first, chip_max, both_max), jnp.where(first, enter_norm, both_norm)
    write_info(finfo_out, jnp.where(first, both_norm, enter_norm), jnp.where(first, both_max, chip_max), a_decay, gate)
    ahead = remote(finfo_out, finfo_in, fi_ss.at[0], fi_rs.at[0], partner)
    ahead.start()
    sends.append(ahead)

    es = []
    for h in range(chunks):
        for copy in ys[h]:
            copy.wait_recv()
        before = jnp.zeros((share, wide), F32)
        for j in range(ny):
            before = y_scales[j][0] * before + y_scales[j][1] * y_in[h, j].astype(F32)
        for j in range(nz):
            e_buf[h, j] = (e_scales[j][0] * before + e_scales[j][1] * p_buf[h, j]).astype(BF16)
        es.append([])
        for d in order:
            peer = lax.rem(z + d, nz)
            copy = remote(e_buf.at[h, peer], e_in.at[h, z], e_ss.at[h, d], e_rs.at[h, d], {"z": peer})
            copy.start()
            es[h].append(copy)
        e_in[h, z] = e_buf[h, z]
        sends += es[h]

    upward, downward = {"y": lax.rem(y + 1, ny)}, {"y": lax.rem(y + ny - 1, ny)}
    w_pair = []

    def to_partner(i, rows, n):
        place = w_buf.at[i, rows, :]
        copy = remote(place, place, wp_ss.at[n, i], wp_rs.at[n, i], partner)
        copy.start()
        w_pair.append(copy)

    wy = [[], []]
    for i in range(3):
        wx[i].wait_recv()
        place = w_buf.at[i, mine_rows, :]
        for way, peer in ((0, upward), (1, downward)):
            copy = remote(place, place, wy_ss.at[way, i], wy_rs.at[way, i], peer)
            copy.start()
            wy[way].append(copy)
        to_partner(i, mine_rows, 0)
    wf = [[], []]

    def pass_weights(i):
        for way, peer, source in ((0, upward, y + ny - 1), (1, downward, y + 1)):
            wy[way][i].wait_recv()
            start = slab_of(lax.rem(source, ny), c)
            place = w_buf.at[i, pl.ds(pl.multiple_of(start + way * (slab // 2), slab // 2), slab // 2), :]
            copy = remote(place, place, wf_ss.at[way, i], wf_rs.at[way, i], peer)
            copy.start()
            wf[way].append(copy)
            to_partner(i, pl.ds(start, slab), 1 + way)

    def factors(s, norm, top):
        for r in range(2):
            rows = pl.ds(r * half, half)
            carried_den = jnp.sum(q_buf[s, rows, :].astype(F32) * norm, axis=1, keepdims=True)
            b_top = bmax_buf[s, rows, :]
            stabilizer = jnp.maximum(b_top, top)
            a, k = jnp.exp(b_top - stabilizer), jnp.exp(top - stabilizer)
            den = a * den_buf[s, rows, :] + k * carried_den
            inverse = 1.0 / jnp.maximum(jnp.abs(den), 1.0)
            bmax_buf[s, rows, :] = a * inverse
            den_buf[s, rows, :] = k * inverse

    factors(1, my_norm, my_max)
    ahead.wait_recv()
    other_norm, other_max, unused_decay, other_gate = read_info(finfo_in, 0)
    scale = 1.0 / (tokens * ny * nz * 2)
    lane = lax.broadcasted_iota(jnp.int32, (1, 2), 1)
    gate_ref[...] = jnp.where(lane == c, gate, other_gate) * scale
    factors(0, other_norm, other_max)

    def readout(s, h, carry):
        for r in range(2):
            rows = pl.ds(r * half, half)
            carried = dot(q_buf[s, rows, :], carry)
            own = num_buf[s, rows, h * wide : (h + 1) * wide]
            hid[s * chunks + h, rows, :] = (bmax_buf[s, rows, :] * own + den_buf[s, rows, :] * carried).astype(BF16)

    ag = [{}, {}]
    sequence = []

    def gather(s, h):
        r = s * chunks + h
        sequence.append(r)
        for way, peer in ((0, right), (1, left)):
            copy = remote(hid.at[r], ag_in.at[way, r], ag_ss.at[way, r], ag_rs.at[way, r], peer)
            copy.start()
            ag[way][r] = copy

    finish = []
    for h in range(chunks):
        for copy in es[h]:
            copy.wait_recv()
        for j in range(nz):
            rows = pl.ds(j * share, share)
            entering = e_in[h, j].astype(F32)
            a_rows = jnp.where(first, own1[rows, h * wide : (h + 1) * wide], pair_in[rows, h * wide : (h + 1) * wide].astype(F32))
            both = e_scale * entering + l_scale * a_rows
            f_out[h, rows, :] = jnp.where(first, both, entering).astype(BF16)
            mine[h, rows, :] = jnp.where(first, entering, both).astype(BF16)
        copy = remote(f_out.at[h], f_in.at[h], f_ss.at[h], f_rs.at[h], partner)
        copy.start()
        finish.append(copy)
        readout(1, h, mine[h])
        gather(1, h)
        if h > 0:
            finish[h - 1].wait_recv()
            readout(0, h - 1, f_in[h - 1])
            gather(0, h - 1)
    sends += finish
    finish[chunks - 1].wait_recv()
    readout(0, chunks - 1, f_in[chunks - 1])
    gather(0, chunks - 1)

    def product(source, i, s, n, low, high):
        hidden = [source[s * chunks + h] for h in range(low, high)]
        left_side = hidden[0] if len(hidden) == 1 else jnp.concatenate(hidden, axis=1)
        rows = pl.ds(pl.multiple_of(heads[s] * dv + low * wide, wide), (high - low) * wide)
        return dot(left_side, w_buf[i, rows, n * step : (n + 1) * step])

    parts = cols // step
    w_own.wait()
    for n in range(parts):
        acc[n] = product(hid, 3, 1, n, 0, chunks) + product(hid, 3, 0, n, 0, chunks)

    passed_on = [{}, {}]

    def pass_hidden(r):
        for way, peer in ((0, right), (1, left)):
            ag[way][r].wait_recv()
            rows = pl.ds(way * half, half)
            copy = remote(ag_in.at[way, r, rows, :], ag_in.at[2, r, rows, :], af_ss.at[way, r], af_rs.at[way, r], peer)
            copy.start()
            passed_on[way][r] = copy

    plan = iter(sequence)
    for i, count in ((0, 1), (1, 2), (2, 2)):
        for _ in range(count):
            pass_hidden(next(plan))
        pass_weights(i)
    for r in plan:
        pass_hidden(r)
    far_rows = pl.ds(slab_of(lax.rem(y + 2, ny), c), slab)
    for i in range(3):
        wf[0][i].wait_recv()
        wf[1][i].wait_recv()
        to_partner(i, far_rows, 3)
    for copy in w_pair:
        copy.wait_recv()
    for n in range(parts):
        acc[n] += (product(ag_in.at[0], 0, 1, n, 0, chunks) + product(ag_in.at[0], 0, 0, n, 0, chunks)) + (
            product(ag_in.at[1], 1, 1, n, 0, chunks) + product(ag_in.at[1], 1, 0, n, 0, chunks)
        )

    def arrived(s, low, high):
        for h in range(low, high):
            for way in range(2):
                passed_on[way][s * chunks + h].wait_recv()

    arrived(1, 0, chunks)
    arrived(0, 0, chunks - 1)
    for n in range(parts):
        acc[n] += product(ag_in.at[2], 2, 1, n, 0, chunks) + product(ag_in.at[2], 2, 0, n, 0, chunks - 1)
    arrived(0, chunks - 1, chunks)
    for n in range(parts):
        mixed_ref[:, n * step : (n + 1) * step] = (acc[n] + product(ag_in.at[2], 2, 0, n, chunks - 1, chunks)).astype(BF16)
    for group in wy + wf + [w_pair]:
        sends += group
    for group in ag + passed_on:
        sends += list(group.values())
    for copy in sends:
        copy.wait_send()


def shards(queries, keys, values, forget_gate, input_gate, out_weight):
    tokens, heads = forget_gate.shape
    dk, dv = queries.shape[1] // heads, values.shape[1] // heads
    width = out_weight.shape[1]
    ny, nz, nx = (lax.axis_size(a) for a in ("y", "z", "x"))
    cols = width // nx
    share = dk // nz
    chunks, step = 4, 256
    wide = dv // chunks
    any_space = pl.BlockSpec(memory_space=pltpu.HBM)
    dma = pltpu.SemaphoreType.DMA
    info = lambda n: pltpu.VMEM((n, 1, INFO), F32)
    mixed, gate_mean = pl.pallas_call(
        functools.partial(kernel, (ny, nz, nx)),
        out_shape=(pltpu.VMEM((tokens, cols), BF16), pltpu.VMEM((1, heads), F32)),
        in_specs=[any_space] * 6,
        out_specs=(pl.BlockSpec(memory_space=pltpu.VMEM), pl.BlockSpec(memory_space=pltpu.VMEM)),
        scratch_shapes=[
            pltpu.VMEM((2, tokens, dk), BF16),
            pltpu.VMEM((2, tokens, dk), BF16),
            pltpu.VMEM((2, tokens, dv), BF16),
            pltpu.VMEM((heads, tokens), F32),
            pltpu.VMEM((heads, tokens), F32),
            pltpu.VMEM((4, heads * dv, cols), BF16),
            pltpu.VMEM((2, dk, tokens), BF16),
            pltpu.VMEM((dk, dv), F32),
            pltpu.VMEM((dk, dv), BF16),
            pltpu.VMEM((dk, dv), BF16),
            info(1),
            info(1),
            pltpu.VMEM((chunks, nz, share, wide), BF16),
            pltpu.VMEM((chunks, nz, share, wide), BF16),
            info(1),
            info(nz),
            pltpu.VMEM((chunks, nz, share, wide), F32),
            pltpu.VMEM((chunks, share, wide), BF16),
            pltpu.VMEM((chunks, ny, share, wide), BF16),
            info(1),
            info(ny),
            pltpu.VMEM((chunks, nz, share, wide), BF16),
            pltpu.VMEM((chunks, nz, share, wide), BF16),
            pltpu.VMEM((chunks, dk, wide), BF16),
            pltpu.VMEM((chunks, dk, wide), BF16),
            info(1),
            info(1),
            pltpu.VMEM((chunks, dk, wide), BF16),
            pltpu.VMEM((2, tokens, dv), F32),
            pltpu.VMEM((2, tokens, 1), F32),
            pltpu.VMEM((2, tokens, 1), F32),
            pltpu.VMEM((2 * chunks, tokens, wide), BF16),
            pltpu.VMEM((3, 2 * chunks, tokens, wide), BF16),
            pltpu.VMEM((cols // step, tokens, step), F32),
            dma((8,)), dma((1,)),
            dma((2,)), dma((2,)),
            dma((chunks, nz)), dma((chunks, nz)), dma((nz,)), dma((nz,)),
            dma((chunks, ny)), dma((chunks, ny)), dma((ny,)), dma((ny,)),
            dma((chunks, nz)), dma((chunks, nz)),
            dma((chunks,)), dma((chunks,)), dma((1,)), dma((1,)),
            dma((3,)), dma((3,)), dma((2, 3)), dma((2, 3)), dma((2, 3)), dma((2, 3)), dma((4, 3)), dma((4, 3)),
            dma((2, 2 * chunks)), dma((2, 2 * chunks)), dma((2, 2 * chunks)), dma((2, 2 * chunks)),
        ],
        compiler_params=pltpu.CompilerParams(
            collective_id=0, has_side_effects=True, vmem_limit_bytes=65000000
        ),
        name="mlstm_layer",
    )(queries, keys, values, forget_gate.T, input_gate.T, out_weight)
    return mixed, gate_mean.reshape(heads)


def solution(mesh):
    torus = Mesh(mesh.devices.reshape(4, 8, 2, mesh.shape["head"]), ("y", "z", "c", "x"))
    both = P(SEQ, "x")
    return jax.shard_map(
        shards,
        mesh=torus,
        in_specs=(both, both, both, both, both, P("x", None)),
        out_specs=(P(SEQ, "x"), P("x")),
        check_vma=False,
    )
```

```python
import functools

import jax
import jax.numpy as jnp
from jax import lax
from jax.experimental import pallas as pl
from jax.experimental.pallas import tpu as pltpu
from jax.sharding import Mesh
from jax.sharding import PartitionSpec as P

MESH = pl.DeviceIdType.MESH
SEQ = ("y", "z", "c")
F32 = jnp.float32
BF16 = jnp.bfloat16
LOW = -1e30
INFO = 384


def dot(a, b):
    return jnp.dot(a, b, preferred_element_type=F32)


def merge(e_max, l_max, l_decay):
    top = jnp.maximum(l_decay + e_max, l_max)
    return jnp.exp(l_decay + e_max - top), jnp.exp(l_max - top), top


def three_rows(row, first):
    hi = row.astype(BF16).astype(F32)
    mid = (row - hi).astype(BF16).astype(F32)
    low = row - hi - mid
    return jnp.where(first == 0, hi, jnp.where(first == 1, mid, jnp.where(first == 2, low, 0.0))).astype(BF16)


def read_info(ref, j):
    row = ref[j]
    return row[:, :256], row[:, 256:257], row[:, 288:289], row[:, 320:321]


def write_info(ref, norm, top, decay, gate):
    lane = lax.broadcasted_iota(jnp.int32, (1, 128), 1)
    ref[0, :, 0:256] = norm
    ref[0, :, 256:384] = jnp.where(lane < 32, top, jnp.where(lane < 64, decay, gate))


def kernel(
    sizes,
    q_hbm, k_hbm, v_hbm, fg_hbm, ig_hbm, w_hbm,
    mixed_ref, gate_ref,
    q_buf, k_buf, v_buf, fg_buf, ig_buf, w_buf, kt_buf, wkt_buf,
    own1, pair_out, pair_in, pinfo_out, pinfo_in,
    t_buf, t_in, tinfo_out, tinfo,
    p_buf, y_out, y_in, yinfo_out, yinfo,
    e_buf, e_in, f_out, f_in, finfo_out, finfo_in, mine,
    num_buf, bmax_buf, den_buf, hid,
    ag_in, acc,
    load_sem, w_sem,
    pair_ss, pair_rs, pi_ss, pi_rs, z_ss, z_rs, zi_ss, zi_rs, y_ss, y_rs, yi_ss, yi_rs, e_ss, e_rs, f_ss, f_rs, fi_ss, fi_rs,
    wx_ss, wx_rs, wy_ss, wy_rs, wf_ss, wf_rs, wp_ss, wp_rs, ag_ss, ag_rs, af_ss, af_rs,
):
    ny, nz, nx = sizes
    y, z, c, x = (lax.axis_index(a) for a in ("y", "z", "c", "x"))
    tokens = q_buf.shape[1]
    dk, dv = q_buf.shape[2], v_buf.shape[2]
    half = tokens // 2
    cols = w_buf.shape[2]
    slab = w_buf.shape[1] // (2 * ny)
    share = dk // nz
    chunks, wide, step = t_buf.shape[0], t_buf.shape[3], acc.shape[2]
    first = c == 0
    heads = (1 - c, c)

    loads = []

    def load(src, dst):
        loads.append(pltpu.make_async_copy(src, dst, load_sem.at[len(loads)]))

    load(fg_hbm, fg_buf)
    load(ig_hbm, ig_buf)
    for s in range(2):
        load(k_hbm.at[:, pl.ds(pl.multiple_of(heads[s] * dk, 128), dk)], k_buf.at[s])
        load(v_hbm.at[:, pl.ds(pl.multiple_of(heads[s] * dv, 128), dv)], v_buf.at[s])
    for s in range(2):
        load(q_hbm.at[:, pl.ds(pl.multiple_of(heads[s] * dk, 128), dk)], q_buf.at[s])

    for copy in loads[:4]:
        copy.start()

    barrier = pltpu.get_barrier_semaphore()
    peers = [{"c": 1 - c}]
    peers += [{"z": lax.rem(z + d, nz)} for d in range(1, nz)]
    peers += [{"y": lax.rem(y + d, ny)} for d in range(1, ny)]
    left, right = {"x": lax.rem(x + nx - 1, nx)}, {"x": lax.rem(x + 1, nx)}
    far = {"x": lax.rem(x + 2, nx)}
    peers += [left, right, far]
    for peer in peers:
        pl.semaphore_signal(barrier, inc=1, device_id=peer, device_id_type=MESH)

    for copy in loads[:3]:
        copy.wait()
    for copy in loads[4:6]:
        copy.start()
    fg, ig = fg_buf[...], ig_buf[...]
    lf = jnp.minimum(fg, 0.0) - jnp.log1p(jnp.exp(-jnp.abs(fg)))
    lf_rows = (jnp.where(first, lf[1:2], lf[0:1]), jnp.where(first, lf[0:1], lf[1:2]))
    ig_rows = (jnp.where(first, ig[1:2], ig[0:1]), jnp.where(first, ig[0:1], ig[1:2]))
    sub = lax.broadcasted_iota(jnp.int32, (8, tokens), 0)
    upper = (
        lax.broadcasted_iota(jnp.int32, (tokens, tokens), 0) <= lax.broadcasted_iota(jnp.int32, (tokens, tokens), 1)
    ).astype(F32).astype(BF16)
    stacked = jnp.where(
        sub < 4,
        three_rows(jnp.broadcast_to(lf_rows[0], (8, tokens)), sub).astype(F32),
        three_rows(jnp.broadcast_to(lf_rows[1], (8, tokens)), sub - 4).astype(F32),
    ).astype(BF16)
    cums = dot(stacked, upper)
    b_rows, decays, tops, weights = [], [], [], []
    for s in range(2):
        cum = jnp.sum(cums[4 * s : 4 * s + 4], axis=0, keepdims=True)
        b = ig_rows[s] - cum
        decay = cum[:, tokens - 1 : tokens]
        b_top = jnp.max(b, axis=1, keepdims=True)
        b_rows.append(b)
        decays.append(decay)
        tops.append(decay + b_top)
        weights.append(jnp.exp(b - b_top) * (dk**-0.5))
    gates = [jnp.sum(ig_rows[s], axis=1, keepdims=True) for s in range(2)]

    def own_keys(s):
        kt = k_buf[s].T
        kt_buf[s] = kt
        wkt_buf[s] = (kt.astype(F32) * weights[s]).astype(BF16)
        return jnp.sum(dot(three_rows(jnp.broadcast_to(weights[s], (8, tokens)), sub), k_buf[s]), axis=0, keepdims=True)

    def own_state(s, h):
        return dot(wkt_buf[s], v_buf[s, :, h * wide : (h + 1) * wide])

    def remote(src, dst, ss, rs, peer):
        return pltpu.make_async_remote_copy(
            src_ref=src, dst_ref=dst, send_sem=ss, recv_sem=rs, device_id=peer, device_id_type=MESH
        )

    sends = []

    norm0 = own_keys(0)
    write_info(pinfo_out, norm0, tops[0], decays[0], gates[0])
    loads[3].wait()
    for copy in loads[6:]:
        copy.start()
    pair_out[0] = own_state(0, 0).astype(BF16)
    pl.semaphore_wait(barrier, len(peers))
    partner = {"c": 1 - c}
    pair_info = remote(pinfo_out, pinfo_in, pi_ss.at[0], pi_rs.at[0], partner)
    pair_info.start()
    pair = []

    def send_pair(h):
        copy = remote(pair_out.at[h], pair_in.at[h], pair_ss.at[h], pair_rs.at[h], partner)
        copy.start()
        pair.append(copy)

    send_pair(0)
    for h in range(1, chunks):
        pair_out[h] = own_state(0, h).astype(BF16)
        send_pair(h)
    sends += [pair_info] + pair

    def slab_of(y_index, c_index):
        return pl.multiple_of((y_index * 2 + c_index) * slab, slab)

    mine_rows = pl.ds(slab_of(y, c), slab)
    wx = []
    for i, peer in ((0, right), (1, left), (2, far)):
        copy = remote(
            w_hbm.at[mine_rows, pl.ds(pl.multiple_of(peer["x"] * cols, 128), cols)], w_buf.at[i, mine_rows, :], wx_ss.at[i], wx_rs.at[i], peer
        )
        copy.start()
        wx.append(copy)
    sends += wx
    w_own = pltpu.make_async_copy(w_hbm.at[:, pl.ds(pl.multiple_of(x * cols, 128), cols)], w_buf.at[3], w_sem.at[0])

    loads[4].wait()
    norm1 = own_keys(1)
    loads[5].wait()
    own1[0] = own_state(1, 0)

    pair_info.wait_recv()
    in_norm, in_top, in_decay, in_gate = read_info(pinfo_in, 0)
    a_top, a_norm = jnp.where(first, tops[1], in_top), jnp.where(first, norm1, in_norm)
    a_decay = jnp.where(first, decays[1], in_decay)
    l_top, l_norm = jnp.where(first, in_top, tops[1]), jnp.where(first, in_norm, norm1)
    l_decay = jnp.where(first, in_decay, decays[1])
    e_scale, l_scale, chip_top = merge(a_top, l_top, l_decay)
    chip_norm = e_scale * a_norm + l_scale * l_norm
    write_info(tinfo_out, chip_norm, chip_top, a_decay + l_decay, gates[1] + in_gate)
    zi = []
    order = sorted(range(1, nz), key=lambda d: -min(d, nz - d))
    for d in order:
        copy = remote(tinfo_out.at[0], tinfo.at[z], zi_ss.at[d], zi_rs.at[d], {"z": lax.rem(z + d, nz)})
        copy.start()
        zi.append(copy)
    tinfo[z] = tinfo_out[0]
    own_scale, in_scale = jnp.where(first, e_scale, l_scale), jnp.where(first, l_scale, e_scale)
    zs = []
    for h in range(chunks):
        if h > 0:
            own1[h] = own_state(1, h)
        pair[h].wait_recv()
        for j in range(nz):
            rows = pl.ds(j * share, share)
            t_buf[h, j] = (own_scale * own1[h, rows, :] + in_scale * pair_in[h, rows, :].astype(F32)).astype(BF16)
        zs.append([])
        for d in order:
            peer = lax.rem(z + d, nz)
            copy = remote(t_buf.at[h, peer], t_in.at[h, z], z_ss.at[h, d], z_rs.at[h, d], {"z": peer})
            copy.start()
            zs[h].append(copy)
        t_in[h, z] = t_buf[h, z]
        sends += zs[h]
    sends += zi

    w_own.start()

    loads[6].wait()
    loads[7].wait()

    def intra(s):
        for r in range(2):
            rows = pl.ds(r * half, half)
            span = half * (r + 1)
            scores = dot(q_buf[s, rows, :], kt_buf[s, :, :span]) * (dk**-0.5)
            t_index = lax.broadcasted_iota(jnp.int32, (half, span), 0) + r * half
            s_index = lax.broadcasted_iota(jnp.int32, (half, span), 1)
            logs = jnp.where(s_index <= t_index, jnp.broadcast_to(b_rows[s][:, :span], (half, span)), -jnp.inf)
            top = jnp.max(logs, axis=1, keepdims=True)
            weighted = jnp.exp(logs - top) * scores
            bmax_buf[s, rows, :] = top
            den_buf[s, rows, :] = jnp.sum(weighted, axis=1, keepdims=True)
            num_buf[s, rows, :] = dot(weighted.astype(BF16), v_buf[s, :span, :])

    intra(1)
    intra(0)

    for copy in zi:
        copy.wait_recv()
    top, decay, norm, gate = jnp.full((1, 1), LOW, F32), jnp.zeros((1, 1), F32), jnp.zeros((1, dk), F32), jnp.zeros((1, 1), F32)
    z_norm, z_top, z_decay = norm, top, decay
    z_tops, z_decays, scales = [], [], []
    for j in range(nz):
        z_tops.append(top)
        z_decays.append(decay)
        here = j == z
        z_norm, z_top, z_decay = jnp.where(here, norm, z_norm), jnp.where(here, top, z_top), jnp.where(here, decay, z_decay)
        j_norm, j_top, j_decay, j_gate = read_info(tinfo, j)
        e_scale, l_scale, top = merge(top, j_top, j_decay)
        norm = e_scale * norm + l_scale * j_norm
        decay = decay + j_decay
        gate = gate + j_gate
        scales.append((e_scale, l_scale))
    write_info(yinfo_out, norm, top, decay, gate)
    yi = []
    y_order = sorted(range(1, ny), key=lambda d: -min(d, ny - d))
    for d in y_order:
        copy = remote(yinfo_out.at[0], yinfo.at[y], yi_ss.at[d], yi_rs.at[d], {"y": lax.rem(y + d, ny)})
        copy.start()
        yi.append(copy)
    yinfo[y] = yinfo_out[0]
    ys = []
    for h in range(chunks):
        for copy in zs[h]:
            copy.wait_recv()
        running = jnp.zeros((share, wide), F32)
        for j in range(nz):
            p_buf[h, j] = running
            running = scales[j][0] * running + scales[j][1] * t_in[h, j].astype(F32)
        y_out[h] = running.astype(BF16)
        ys.append([])
        for d in y_order:
            copy = remote(y_out.at[h], y_in.at[h, y], y_ss.at[h, d], y_rs.at[h, d], {"y": lax.rem(y + d, ny)})
            copy.start()
            ys[h].append(copy)
        y_in[h, y] = y_out[h]
        sends += ys[h]
    sends += yi

    for copy in yi:
        copy.wait_recv()
    top, decay, norm, gate = jnp.full((1, 1), LOW, F32), jnp.zeros((1, 1), F32), jnp.zeros((1, dk), F32), jnp.zeros((1, 1), F32)
    y_scales = []
    for j in range(ny):
        j_norm, j_top, j_decay, j_gate = read_info(yinfo, j)
        passed = j < y
        e_scale, l_scale, next_top = merge(top, j_top, j_decay)
        norm = jnp.where(passed, e_scale * norm + l_scale * j_norm, norm)
        top = jnp.where(passed, next_top, top)
        gate = gate + j_gate
        y_scales.append((jnp.where(passed, e_scale, 1.0), jnp.where(passed, l_scale, 0.0)))
    e_scales = [merge(top, z_tops[j], z_decays[j]) for j in range(nz)]
    e_scale, l_scale, chip_max = merge(top, z_top, z_decay)
    enter_norm = e_scale * norm + l_scale * z_norm

    e_scale, l_scale, both_max = merge(chip_max, a_top, a_decay)
    both_norm = e_scale * enter_norm + l_scale * a_norm
    my_max, my_norm = jnp.where(first, chip_max, both_max), jnp.where(first, enter_norm, both_norm)
    write_info(finfo_out, jnp.where(first, both_norm, enter_norm), jnp.where(first, both_max, chip_max), a_decay, gate)
    ahead = remote(finfo_out, finfo_in, fi_ss.at[0], fi_rs.at[0], partner)
    ahead.start()
    sends.append(ahead)

    es = []
    for h in range(chunks):
        for copy in ys[h]:
            copy.wait_recv()
        before = jnp.zeros((share, wide), F32)
        for j in range(ny):
            before = y_scales[j][0] * before + y_scales[j][1] * y_in[h, j].astype(F32)
        for j in range(nz):
            e_buf[h, j] = (e_scales[j][0] * before + e_scales[j][1] * p_buf[h, j]).astype(BF16)
        es.append([])
        for d in order:
            peer = lax.rem(z + d, nz)
            copy = remote(e_buf.at[h, peer], e_in.at[h, z], e_ss.at[h, d], e_rs.at[h, d], {"z": peer})
            copy.start()
            es[h].append(copy)
        e_in[h, z] = e_buf[h, z]
        sends += es[h]

    upward, downward = {"y": lax.rem(y + 1, ny)}, {"y": lax.rem(y + ny - 1, ny)}
    w_pair = []

    def to_partner(i, rows, n):
        place = w_buf.at[i, rows, :]
        copy = remote(place, place, wp_ss.at[n, i], wp_rs.at[n, i], partner)
        copy.start()
        w_pair.append(copy)

    wy = [[], []]
    for i in range(3):
        wx[i].wait_recv()
        place = w_buf.at[i, mine_rows, :]
        for way, peer in ((0, upward), (1, downward)):
            copy = remote(place, place, wy_ss.at[way, i], wy_rs.at[way, i], peer)
            copy.start()
            wy[way].append(copy)
        to_partner(i, mine_rows, 0)
    wf = [[], []]

    def pass_weights(i):
        for way, peer, source in ((0, upward, y + ny - 1), (1, downward, y + 1)):
            wy[way][i].wait_recv()
            start = slab_of(lax.rem(source, ny), c)
            place = w_buf.at[i, pl.ds(pl.multiple_of(start + way * (slab // 2), slab // 2), slab // 2), :]
            copy = remote(place, place, wf_ss.at[way, i], wf_rs.at[way, i], peer)
            copy.start()
            wf[way].append(copy)
            to_partner(i, pl.ds(start, slab), 1 + way)

    def factors(s, norm, top):
        for r in range(2):
            rows = pl.ds(r * half, half)
            carried_den = jnp.sum(q_buf[s, rows, :].astype(F32) * norm, axis=1, keepdims=True)
            b_top = bmax_buf[s, rows, :]
            stabilizer = jnp.maximum(b_top, top)
            a, k = jnp.exp(b_top - stabilizer), jnp.exp(top - stabilizer)
            den = a * den_buf[s, rows, :] + k * carried_den
            inverse = 1.0 / jnp.maximum(jnp.abs(den), 1.0)
            bmax_buf[s, rows, :] = a * inverse
            den_buf[s, rows, :] = k * inverse

    factors(1, my_norm, my_max)
    ahead.wait_recv()
    other_norm, other_max, unused_decay, other_gate = read_info(finfo_in, 0)
    scale = 1.0 / (tokens * ny * nz * 2)
    lane = lax.broadcasted_iota(jnp.int32, (1, 2), 1)
    gate_ref[...] = jnp.where(lane == c, gate, other_gate) * scale
    factors(0, other_norm, other_max)

    def readout(s, h, carry):
        for r in range(2):
            rows = pl.ds(r * half, half)
            carried = dot(q_buf[s, rows, :], carry)
            own = num_buf[s, rows, h * wide : (h + 1) * wide]
            hid[s * chunks + h, rows, :] = (bmax_buf[s, rows, :] * own + den_buf[s, rows, :] * carried).astype(BF16)

    ag = [{}, {}]
    sequence = []

    def gather(s, h):
        r = s * chunks + h
        sequence.append(r)
        for way, peer in ((0, right), (1, left)):
            copy = remote(hid.at[r], ag_in.at[way, r], ag_ss.at[way, r], ag_rs.at[way, r], peer)
            copy.start()
            ag[way][r] = copy

    finish = []
    for h in range(chunks):
        for copy in es[h]:
            copy.wait_recv()
        for j in range(nz):
            rows = pl.ds(j * share, share)
            entering = e_in[h, j].astype(F32)
            a_rows = jnp.where(first, own1[h, rows, :], pair_in[h, rows, :].astype(F32))
            both = e_scale * entering + l_scale * a_rows
            f_out[h, rows, :] = jnp.where(first, both, entering).astype(BF16)
            mine[h, rows, :] = jnp.where(first, entering, both).astype(BF16)
        copy = remote(f_out.at[h], f_in.at[h], f_ss.at[h], f_rs.at[h], partner)
        copy.start()
        finish.append(copy)
        readout(1, h, mine[h])
        gather(1, h)
        if h > 0:
            finish[h - 1].wait_recv()
            readout(0, h - 1, f_in[h - 1])
            gather(0, h - 1)
    sends += finish
    finish[chunks - 1].wait_recv()
    readout(0, chunks - 1, f_in[chunks - 1])
    gather(0, chunks - 1)

    def product(source, i, s, n, low, high):
        hidden = [source[s * chunks + h] for h in range(low, high)]
        left_side = hidden[0] if len(hidden) == 1 else jnp.concatenate(hidden, axis=1)
        rows = pl.ds(pl.multiple_of(heads[s] * dv + low * wide, wide), (high - low) * wide)
        return dot(left_side, w_buf[i, rows, n * step : (n + 1) * step])

    parts = cols // step
    w_own.wait()
    for n in range(parts):
        acc[n] = product(hid, 3, 1, n, 0, chunks) + product(hid, 3, 0, n, 0, chunks)

    passed_on = [{}, {}]

    def pass_hidden(r):
        for way, peer in ((0, right), (1, left)):
            ag[way][r].wait_recv()
            rows = pl.ds(way * half, half)
            copy = remote(ag_in.at[way, r, rows, :], ag_in.at[2, r, rows, :], af_ss.at[way, r], af_rs.at[way, r], peer)
            copy.start()
            passed_on[way][r] = copy

    plan = iter(sequence)
    for i, count in ((0, 1), (1, 2), (2, 2)):
        for _ in range(count):
            pass_hidden(next(plan))
        pass_weights(i)
    for r in plan:
        pass_hidden(r)
    far_rows = pl.ds(slab_of(lax.rem(y + 2, ny), c), slab)
    for i in range(3):
        wf[0][i].wait_recv()
        wf[1][i].wait_recv()
        to_partner(i, far_rows, 3)
    for copy in w_pair:
        copy.wait_recv()
    for n in range(parts):
        acc[n] += (product(ag_in.at[0], 0, 1, n, 0, chunks) + product(ag_in.at[0], 0, 0, n, 0, chunks)) + (
            product(ag_in.at[1], 1, 1, n, 0, chunks) + product(ag_in.at[1], 1, 0, n, 0, chunks)
        )

    def arrived(s, low, high):
        for h in range(low, high):
            for way in range(2):
                passed_on[way][s * chunks + h].wait_recv()

    arrived(1, 0, chunks)
    arrived(0, 0, chunks - 1)
    for n in range(parts):
        acc[n] += product(ag_in.at[2], 2, 1, n, 0, chunks) + product(ag_in.at[2], 2, 0, n, 0, chunks - 1)
    arrived(0, chunks - 1, chunks)
    for n in range(parts):
        mixed_ref[:, n * step : (n + 1) * step] = (acc[n] + product(ag_in.at[2], 2, 0, n, chunks - 1, chunks)).astype(BF16)
    for group in wy + wf + [w_pair]:
        sends += group
    for group in ag + passed_on:
        sends += list(group.values())
    for copy in sends:
        copy.wait_send()


def put_out(mixed_ref, gate_ref, mixed_hbm, gate_hbm, sems):
    copies = [pltpu.make_async_copy(mixed_ref, mixed_hbm, sems.at[0]), pltpu.make_async_copy(gate_ref, gate_hbm, sems.at[1])]
    for copy in copies:
        copy.start()
    for copy in copies:
        copy.wait()


def shards(queries, keys, values, forget_gate, input_gate, out_weight):
    tokens, heads = forget_gate.shape
    dk, dv = queries.shape[1] // heads, values.shape[1] // heads
    width = out_weight.shape[1]
    ny, nz, nx = (lax.axis_size(a) for a in ("y", "z", "x"))
    cols = width // nx
    share = dk // nz
    chunks, step = 4, 256
    wide = dv // chunks
    any_space = pl.BlockSpec(memory_space=pltpu.HBM)
    dma = pltpu.SemaphoreType.DMA
    info = lambda n: pltpu.VMEM((n, 1, INFO), F32)
    mixed, gate_mean = pl.pallas_call(
        functools.partial(kernel, (ny, nz, nx)),
        out_shape=(pltpu.VMEM((tokens, cols), BF16), pltpu.VMEM((1, heads), F32)),
        in_specs=[any_space] * 6,
        out_specs=(pl.BlockSpec(memory_space=pltpu.VMEM), pl.BlockSpec(memory_space=pltpu.VMEM)),
        scratch_shapes=[
            pltpu.VMEM((2, tokens, dk), BF16),
            pltpu.VMEM((2, tokens, dk), BF16),
            pltpu.VMEM((2, tokens, dv), BF16),
            pltpu.VMEM((heads, tokens), F32),
            pltpu.VMEM((heads, tokens), F32),
            pltpu.VMEM((4, heads * dv, cols), BF16),
            pltpu.VMEM((2, dk, tokens), BF16),
            pltpu.VMEM((2, dk, tokens), BF16),
            pltpu.VMEM((chunks, dk, wide), F32),
            pltpu.VMEM((chunks, dk, wide), BF16),
            pltpu.VMEM((chunks, dk, wide), BF16),
            info(1),
            info(1),
            pltpu.VMEM((chunks, nz, share, wide), BF16),
            pltpu.VMEM((chunks, nz, share, wide), BF16),
            info(1),
            info(nz),
            pltpu.VMEM((chunks, nz, share, wide), F32),
            pltpu.VMEM((chunks, share, wide), BF16),
            pltpu.VMEM((chunks, ny, share, wide), BF16),
            info(1),
            info(ny),
            pltpu.VMEM((chunks, nz, share, wide), BF16),
            pltpu.VMEM((chunks, nz, share, wide), BF16),
            pltpu.VMEM((chunks, dk, wide), BF16),
            pltpu.VMEM((chunks, dk, wide), BF16),
            info(1),
            info(1),
            pltpu.VMEM((chunks, dk, wide), BF16),
            pltpu.VMEM((2, tokens, dv), F32),
            pltpu.VMEM((2, tokens, 1), F32),
            pltpu.VMEM((2, tokens, 1), F32),
            pltpu.VMEM((2 * chunks, tokens, wide), BF16),
            pltpu.VMEM((3, 2 * chunks, tokens, wide), BF16),
            pltpu.VMEM((cols // step, tokens, step), F32),
            dma((8,)), dma((1,)),
            dma((chunks,)), dma((chunks,)), dma((1,)), dma((1,)),
            dma((chunks, nz)), dma((chunks, nz)), dma((nz,)), dma((nz,)),
            dma((chunks, ny)), dma((chunks, ny)), dma((ny,)), dma((ny,)),
            dma((chunks, nz)), dma((chunks, nz)),
            dma((chunks,)), dma((chunks,)), dma((1,)), dma((1,)),
            dma((3,)), dma((3,)), dma((2, 3)), dma((2, 3)), dma((2, 3)), dma((2, 3)), dma((4, 3)), dma((4, 3)),
            dma((2, 2 * chunks)), dma((2, 2 * chunks)), dma((2, 2 * chunks)), dma((2, 2 * chunks)),
        ],
        compiler_params=pltpu.CompilerParams(
            collective_id=0, has_side_effects=True, vmem_limit_bytes=65000000
        ),
        name="mlstm_layer",
    )(queries, keys, values, forget_gate.T, input_gate.T, out_weight)
    in_vmem = pl.BlockSpec(memory_space=pltpu.VMEM)
    mixed, gate_mean = pl.pallas_call(
        put_out,
        out_shape=(jax.ShapeDtypeStruct((tokens, cols), BF16), jax.ShapeDtypeStruct((1, heads), F32)),
        in_specs=[in_vmem, in_vmem],
        out_specs=(any_space, any_space),
        scratch_shapes=[dma((2,))],
        compiler_params=pltpu.CompilerParams(vmem_limit_bytes=4 * 1024 * 1024),
        name="put_out",
    )(mixed, gate_mean)
    return mixed, gate_mean.reshape(heads)


def solution(mesh):
    torus = Mesh(mesh.devices.reshape(4, 8, 2, mesh.shape["head"]), ("y", "z", "c", "x"))
    both = P(SEQ, "x")
    return jax.shard_map(
        shards,
        mesh=torus,
        in_specs=(both, both, both, both, both, P("x", None)),
        out_specs=(P(SEQ, "x"), P("x")),
        check_vma=False,
    )
```

```python
import functools

import jax
import jax.numpy as jnp
from jax import lax
from jax.experimental import pallas as pl
from jax.experimental.pallas import tpu as pltpu
from jax.sharding import Mesh
from jax.sharding import PartitionSpec as P

MESH = pl.DeviceIdType.MESH
SEQ = ("y", "z", "c")
F32 = jnp.float32
BF16 = jnp.bfloat16
LOW = -1e30
INFO = 384


def dot(a, b):
    return jnp.dot(a, b, preferred_element_type=F32)


def merge(e_max, l_max, l_decay):
    top = jnp.maximum(l_decay + e_max, l_max)
    return jnp.exp(l_decay + e_max - top), jnp.exp(l_max - top), top


def three_rows(row, first):
    hi = row.astype(BF16).astype(F32)
    mid = (row - hi).astype(BF16).astype(F32)
    low = row - hi - mid
    return jnp.where(first == 0, hi, jnp.where(first == 1, mid, jnp.where(first == 2, low, 0.0))).astype(BF16)


def read_info(ref, j):
    row = ref[j]
    return row[:, :256], row[:, 256:257], row[:, 288:289], row[:, 320:321]


def write_info(ref, norm, top, decay, gate):
    lane = lax.broadcasted_iota(jnp.int32, (1, 128), 1)
    ref[0, :, 0:256] = norm
    ref[0, :, 256:384] = jnp.where(lane < 32, top, jnp.where(lane < 64, decay, gate))


def kernel(
    sizes,
    q_hbm, k_hbm, v_hbm, fg_hbm, ig_hbm, w_hbm,
    mixed_ref, gate_ref,
    q_buf, k_buf, v_buf, fg_buf, ig_buf, w_buf, kt_buf, wkt_buf, upper,
    own1, pair_out, pair_in, pinfo_out, pinfo_in,
    t_buf, t_in, tinfo_out, tinfo,
    p_buf, y_out, y_in, yinfo_out, yinfo,
    e_buf, e_in, f_out, f_in, finfo_out, finfo_in, mine,
    num_buf, bmax_buf, den_buf, hid,
    ag_in, acc,
    load_sem, w_sem,
    one_ss, one_rs, group_ss, group_rs, pair_rs, z_rs, y_rs, e_rs, f_rs, wy_rs, ag_rs, af_rs,
):
    ny, nz, nx = sizes
    y, z, c, x = (lax.axis_index(a) for a in ("y", "z", "c", "x"))
    tokens = q_buf.shape[1]
    dk, dv = q_buf.shape[2], v_buf.shape[2]
    half = tokens // 2
    cols = w_buf.shape[2]
    slab = w_buf.shape[1] // (2 * ny)
    share = dk // nz
    chunks, wide, step = t_buf.shape[0], t_buf.shape[3], acc.shape[2]
    first = c == 0
    partner = {"c": 1 - c}
    heads = (1 - c, c)

    loads = []

    def load(src, dst):
        loads.append(pltpu.make_async_copy(src, dst, load_sem.at[len(loads)]))

    load(fg_hbm, fg_buf)
    load(ig_hbm, ig_buf)
    for s in range(2):
        load(k_hbm.at[:, pl.ds(pl.multiple_of(heads[s] * dk, 128), dk)], k_buf.at[s])
        load(v_hbm.at[:, pl.ds(pl.multiple_of(heads[s] * dv, 128), dv)], v_buf.at[s])
    for s in range(2):
        load(q_hbm.at[:, pl.ds(pl.multiple_of(heads[s] * dk, 128), dk)], q_buf.at[s])

    for copy in loads[:4]:
        copy.start()

    barrier = pltpu.get_barrier_semaphore()
    peers = [{"c": 1 - c}]
    peers += [{"z": lax.rem(z + d, nz)} for d in range(1, nz)]
    peers += [{"y": lax.rem(y + d, ny)} for d in range(1, ny)]
    left, right = {"x": lax.rem(x + nx - 1, nx)}, {"x": lax.rem(x + 1, nx)}
    far = {"x": lax.rem(x + 2, nx)}
    peers += [left, right, far]
    for peer in peers:
        pl.semaphore_signal(barrier, inc=1, device_id=peer, device_id_type=MESH)

    upper[...] = (
        (lax.broadcasted_iota(jnp.int32, (tokens, tokens), 0) <= lax.broadcasted_iota(jnp.int32, (tokens, tokens), 1))
        .astype(F32)
        .astype(BF16)
    )
    for copy in loads[:3]:
        copy.wait()
    for copy in loads[4:6]:
        copy.start()
    fg, ig = fg_buf[...], ig_buf[...]
    lf = jnp.minimum(fg, 0.0) - jnp.log1p(jnp.exp(-jnp.abs(fg)))
    lf_rows = (jnp.where(first, lf[1:2], lf[0:1]), jnp.where(first, lf[0:1], lf[1:2]))
    ig_rows = (jnp.where(first, ig[1:2], ig[0:1]), jnp.where(first, ig[0:1], ig[1:2]))
    sub = lax.broadcasted_iota(jnp.int32, (8, tokens), 0)
    stacked = jnp.where(
        sub < 4,
        three_rows(jnp.broadcast_to(lf_rows[0], (8, tokens)), sub).astype(F32),
        three_rows(jnp.broadcast_to(lf_rows[1], (8, tokens)), sub - 4).astype(F32),
    ).astype(BF16)
    cums = dot(stacked, upper[...])
    b_rows, decays, tops, weights = [], [], [], []
    for s in range(2):
        cum = jnp.sum(cums[4 * s : 4 * s + 4], axis=0, keepdims=True)
        b = ig_rows[s] - cum
        decay = cum[:, tokens - 1 : tokens]
        b_top = jnp.max(b, axis=1, keepdims=True)
        b_rows.append(b)
        decays.append(decay)
        tops.append(decay + b_top)
        weights.append(jnp.exp(b - b_top) * (dk**-0.5))
    gates = [jnp.sum(ig_rows[s], axis=1, keepdims=True) for s in range(2)]

    def own_keys(s):
        kt = k_buf[s].T
        kt_buf[s] = kt
        wkt_buf[s] = (kt.astype(F32) * weights[s]).astype(BF16)
        return jnp.sum(dot(three_rows(jnp.broadcast_to(weights[s], (8, tokens)), sub), k_buf[s]), axis=0, keepdims=True)

    def own_state(s, h):
        return dot(wkt_buf[s], v_buf[s, :, h * wide : (h + 1) * wide])

    def remote(src, dst, ss, rs, peer):
        return pltpu.make_async_remote_copy(
            src_ref=src, dst_ref=dst, send_sem=ss, recv_sem=rs, device_id=peer, device_id_type=MESH
        )

    def landed(place, sem):
        remote(place, place, sem, sem, partner).wait_recv()

    def left_here(place, sem):
        remote(place, place, sem, sem, partner).wait_send()

    norm0 = own_keys(0)
    write_info(pinfo_out, norm0, tops[0], decays[0], gates[0])
    loads[3].wait()
    for copy in loads[6:]:
        copy.start()
    pair_out[0] = own_state(0, 0).astype(BF16)
    pl.semaphore_wait(barrier, len(peers))
    pair_info = remote(pinfo_out, pinfo_in, one_ss.at[0], one_rs.at[0], partner)
    pair_info.start()
    pair = []

    def send_pair(h):
        copy = remote(pair_out.at[h], pair_in.at[h], group_ss.at[0], pair_rs.at[h], partner)
        copy.start()
        pair.append(copy)

    send_pair(0)
    for h in range(1, chunks):
        pair_out[h] = own_state(0, h).astype(BF16)
        send_pair(h)

    def slab_of(y_index, c_index):
        return pl.multiple_of((y_index * 2 + c_index) * slab, slab)

    mine_rows = pl.ds(slab_of(y, c), slab)
    for i, peer in ((0, right), (1, left), (2, far)):
        copy = remote(
            w_hbm.at[mine_rows, pl.ds(pl.multiple_of(peer["x"] * cols, 128), cols)], w_buf.at[i, mine_rows, :], group_ss.at[1], group_rs.at[0], peer
        )
        copy.start()
    w_own = pltpu.make_async_copy(w_hbm.at[:, pl.ds(pl.multiple_of(x * cols, 128), cols)], w_buf.at[3], w_sem.at[0])

    loads[4].wait()
    norm1 = own_keys(1)
    loads[5].wait()
    own1[0] = own_state(1, 0)

    pair_info.wait_recv()
    in_norm, in_top, in_decay, in_gate = read_info(pinfo_in, 0)
    a_top, a_norm = jnp.where(first, tops[1], in_top), jnp.where(first, norm1, in_norm)
    a_decay = jnp.where(first, decays[1], in_decay)
    l_top, l_norm = jnp.where(first, in_top, tops[1]), jnp.where(first, in_norm, norm1)
    l_decay = jnp.where(first, in_decay, decays[1])
    e_scale, l_scale, chip_top = merge(a_top, l_top, l_decay)
    chip_norm = e_scale * a_norm + l_scale * l_norm
    write_info(tinfo_out, chip_norm, chip_top, a_decay + l_decay, gates[1] + in_gate)
    order = sorted(range(1, nz), key=lambda d: -min(d, nz - d))
    for d in order:
        copy = remote(tinfo_out.at[0], tinfo.at[z], group_ss.at[2], group_rs.at[1], {"z": lax.rem(z + d, nz)})
        copy.start()
    tinfo[z] = tinfo_out[0]
    own_scale, in_scale = jnp.where(first, e_scale, l_scale), jnp.where(first, l_scale, e_scale)
    loads[6].wait()
    loads[7].wait()

    def intra(s):
        for r in range(2):
            rows = pl.ds(r * half, half)
            span = half * (r + 1)
            scores = dot(q_buf[s, rows, :], kt_buf[s, :, :span]) * (dk**-0.5)
            t_index = lax.broadcasted_iota(jnp.int32, (half, span), 0) + r * half
            s_index = lax.broadcasted_iota(jnp.int32, (half, span), 1)
            logs = jnp.where(s_index <= t_index, jnp.broadcast_to(b_rows[s][:, :span], (half, span)), -jnp.inf)
            top = jnp.max(logs, axis=1, keepdims=True)
            weighted = jnp.exp(logs - top) * scores
            bmax_buf[s, rows, :] = top
            den_buf[s, rows, :] = jnp.sum(weighted, axis=1, keepdims=True)
            num_buf[s, rows, :] = dot(weighted.astype(BF16), v_buf[s, :span, :])

    @pl.when(c == 0)
    def _():
        intra(1)

    for h in range(chunks):
        if h > 0:
            own1[h] = own_state(1, h)
        pair[h].wait_recv()
        for j in range(nz):
            rows = pl.ds(j * share, share)
            t_buf[h, j] = (own_scale * own1[h, rows, :] + in_scale * pair_in[h, rows, :].astype(F32)).astype(BF16)
        for d in order:
            peer = lax.rem(z + d, nz)
            copy = remote(t_buf.at[h, peer], t_in.at[h, z], group_ss.at[3], z_rs.at[h], {"z": peer})
            copy.start()
        t_in[h, z] = t_buf[h, z]

    w_own.start()

    @pl.when(c == 1)
    def _():
        intra(1)

    intra(0)

    landed(tinfo.at[: nz - 1], group_rs.at[1])
    top, decay, norm, gate = jnp.full((1, 1), LOW, F32), jnp.zeros((1, 1), F32), jnp.zeros((1, dk), F32), jnp.zeros((1, 1), F32)
    z_norm, z_top, z_decay = norm, top, decay
    z_tops, z_decays, scales = [], [], []
    for j in range(nz):
        z_tops.append(top)
        z_decays.append(decay)
        here = j == z
        z_norm, z_top, z_decay = jnp.where(here, norm, z_norm), jnp.where(here, top, z_top), jnp.where(here, decay, z_decay)
        j_norm, j_top, j_decay, j_gate = read_info(tinfo, j)
        e_scale, l_scale, top = merge(top, j_top, j_decay)
        norm = e_scale * norm + l_scale * j_norm
        decay = decay + j_decay
        gate = gate + j_gate
        scales.append((e_scale, l_scale))
    write_info(yinfo_out, norm, top, decay, gate)
    y_order = sorted(range(1, ny), key=lambda d: -min(d, ny - d))
    for d in y_order:
        copy = remote(yinfo_out.at[0], yinfo.at[y], group_ss.at[4], group_rs.at[2], {"y": lax.rem(y + d, ny)})
        copy.start()
    yinfo[y] = yinfo_out[0]
    for h in range(chunks):
        landed(t_in.at[h, : nz - 1], z_rs.at[h])
        running = jnp.zeros((share, wide), F32)
        for j in range(nz):
            p_buf[h, j] = running
            running = scales[j][0] * running + scales[j][1] * t_in[h, j].astype(F32)
        y_out[h] = running.astype(BF16)
        for d in y_order:
            copy = remote(y_out.at[h], y_in.at[h, y], group_ss.at[5], y_rs.at[h], {"y": lax.rem(y + d, ny)})
            copy.start()
        y_in[h, y] = y_out[h]

    landed(yinfo.at[: ny - 1], group_rs.at[2])
    top, decay, norm, gate = jnp.full((1, 1), LOW, F32), jnp.zeros((1, 1), F32), jnp.zeros((1, dk), F32), jnp.zeros((1, 1), F32)
    y_scales = []
    for j in range(ny):
        j_norm, j_top, j_decay, j_gate = read_info(yinfo, j)
        passed = j < y
        e_scale, l_scale, next_top = merge(top, j_top, j_decay)
        norm = jnp.where(passed, e_scale * norm + l_scale * j_norm, norm)
        top = jnp.where(passed, next_top, top)
        gate = gate + j_gate
        y_scales.append((jnp.where(passed, e_scale, 1.0), jnp.where(passed, l_scale, 0.0)))
    e_scales = [merge(top, z_tops[j], z_decays[j]) for j in range(nz)]
    e_scale, l_scale, chip_max = merge(top, z_top, z_decay)
    enter_norm = e_scale * norm + l_scale * z_norm

    e_scale, l_scale, both_max = merge(chip_max, a_top, a_decay)
    both_norm = e_scale * enter_norm + l_scale * a_norm
    my_max, my_norm = jnp.where(first, chip_max, both_max), jnp.where(first, enter_norm, both_norm)
    write_info(finfo_out, jnp.where(first, both_norm, enter_norm), jnp.where(first, both_max, chip_max), a_decay, gate)
    ahead = remote(finfo_out, finfo_in, one_ss.at[1], one_rs.at[1], partner)
    ahead.start()

    for h in range(chunks):
        landed(y_in.at[h, : ny - 1], y_rs.at[h])
        before = jnp.zeros((share, wide), F32)
        for j in range(ny):
            before = y_scales[j][0] * before + y_scales[j][1] * y_in[h, j].astype(F32)
        for j in range(nz):
            e_buf[h, j] = (e_scales[j][0] * before + e_scales[j][1] * p_buf[h, j]).astype(BF16)
        for d in order:
            peer = lax.rem(z + d, nz)
            copy = remote(e_buf.at[h, peer], e_in.at[h, z], group_ss.at[6], e_rs.at[h], {"z": peer})
            copy.start()
        e_in[h, z] = e_buf[h, z]

    upward, downward = {"y": lax.rem(y + 1, ny)}, {"y": lax.rem(y + ny - 1, ny)}
    def to_partner(i, rows):
        place = w_buf.at[i, rows, :]
        remote(place, place, group_ss.at[7], group_rs.at[3], partner).start()

    wy = [[], []]
    landed(w_buf.at[:3, :slab, :], group_rs.at[0])
    for i in range(3):
        place = w_buf.at[i, mine_rows, :]
        for way, peer in ((0, upward), (1, downward)):
            copy = remote(place, place, group_ss.at[8], wy_rs.at[way, i], peer)
            copy.start()
            wy[way].append(copy)
        to_partner(i, mine_rows)

    def pass_weights(i):
        for way, peer, source in ((0, upward, y + ny - 1), (1, downward, y + 1)):
            wy[way][i].wait_recv()
            start = slab_of(lax.rem(source, ny), c)
            place = w_buf.at[i, pl.ds(pl.multiple_of(start + way * (slab // 2), slab // 2), slab // 2), :]
            copy = remote(place, place, group_ss.at[9], group_rs.at[4], peer)
            copy.start()
            to_partner(i, pl.ds(start, slab))

    def factors(s, norm, top):
        for r in range(2):
            rows = pl.ds(r * half, half)
            carried_den = jnp.sum(q_buf[s, rows, :].astype(F32) * norm, axis=1, keepdims=True)
            b_top = bmax_buf[s, rows, :]
            stabilizer = jnp.maximum(b_top, top)
            a, k = jnp.exp(b_top - stabilizer), jnp.exp(top - stabilizer)
            den = a * den_buf[s, rows, :] + k * carried_den
            inverse = 1.0 / jnp.maximum(jnp.abs(den), 1.0)
            bmax_buf[s, rows, :] = a * inverse
            den_buf[s, rows, :] = k * inverse

    factors(1, my_norm, my_max)
    ahead.wait_recv()
    other_norm, other_max, unused_decay, other_gate = read_info(finfo_in, 0)
    scale = 1.0 / (tokens * ny * nz * 2)
    lane = lax.broadcasted_iota(jnp.int32, (1, 2), 1)
    gate_ref[...] = jnp.where(lane == c, gate, other_gate) * scale
    factors(0, other_norm, other_max)

    def readout(s, h, carry):
        for r in range(2):
            rows = pl.ds(r * half, half)
            carried = dot(q_buf[s, rows, :], carry)
            own = num_buf[s, rows, h * wide : (h + 1) * wide]
            hid[s * chunks + h, rows, :] = (bmax_buf[s, rows, :] * own + den_buf[s, rows, :] * carried).astype(BF16)

    ag = [{}, {}]
    sequence = []

    def gather(s, h):
        r = s * chunks + h
        sequence.append(r)
        for way, peer in ((0, right), (1, left)):
            copy = remote(hid.at[r], ag_in.at[way, r], group_ss.at[10], ag_rs.at[way, r], peer)
            copy.start()
            ag[way][r] = copy

    finish = []
    for h in range(chunks):
        landed(e_in.at[h, : nz - 1], e_rs.at[h])
        for j in range(nz):
            rows = pl.ds(j * share, share)
            entering = e_in[h, j].astype(F32)
            a_rows = jnp.where(first, own1[h, rows, :], pair_in[h, rows, :].astype(F32))
            both = e_scale * entering + l_scale * a_rows
            f_out[h, rows, :] = jnp.where(first, both, entering).astype(BF16)
            mine[h, rows, :] = jnp.where(first, entering, both).astype(BF16)
        copy = remote(f_out.at[h], f_in.at[h], group_ss.at[11], f_rs.at[h], partner)
        copy.start()
        finish.append(copy)
        readout(1, h, mine[h])
        gather(1, h)
        if h > 0:
            finish[h - 1].wait_recv()
            readout(0, h - 1, f_in[h - 1])
            gather(0, h - 1)
    finish[chunks - 1].wait_recv()
    readout(0, chunks - 1, f_in[chunks - 1])
    gather(0, chunks - 1)

    def product(source, i, s, n, low, high):
        hidden = [source[s * chunks + h] for h in range(low, high)]
        left_side = hidden[0] if len(hidden) == 1 else jnp.concatenate(hidden, axis=1)
        rows = pl.ds(pl.multiple_of(heads[s] * dv + low * wide, wide), (high - low) * wide)
        return dot(left_side, w_buf[i, rows, n * step : (n + 1) * step])

    parts = cols // step
    w_own.wait()
    for n in range(parts):
        acc[n] = product(hid, 3, 1, n, 0, chunks) + product(hid, 3, 0, n, 0, chunks)

    last = chunks - 1

    def pass_hidden(r):
        group = 0 if r >= chunks else 2 if r == last else 1
        for way, peer in ((0, right), (1, left)):
            ag[way][r].wait_recv()
            rows = pl.ds(way * half, half)
            copy = remote(ag_in.at[way, r, rows, :], ag_in.at[2, r, rows, :], group_ss.at[12], af_rs.at[group], peer)
            copy.start()

    plan = iter(sequence)
    for i, count in ((0, 1), (1, 2), (2, 2)):
        for _ in range(count):
            pass_hidden(next(plan))
        pass_weights(i)
    for r in plan:
        pass_hidden(r)
    far_rows = pl.ds(slab_of(lax.rem(y + 2, ny), c), slab)
    landed(w_buf.at[:3, :slab, :], group_rs.at[4])
    for i in range(3):
        to_partner(i, far_rows)
    landed(w_buf.at[:3, : ny * slab, :], group_rs.at[3])
    for n in range(parts):
        acc[n] += (product(ag_in.at[0], 0, 1, n, 0, chunks) + product(ag_in.at[0], 0, 0, n, 0, chunks)) + (
            product(ag_in.at[1], 1, 1, n, 0, chunks) + product(ag_in.at[1], 1, 0, n, 0, chunks)
        )

    landed(ag_in.at[2, :chunks], af_rs.at[0])
    landed(ag_in.at[2, :last], af_rs.at[1])
    for n in range(parts):
        acc[n] += product(ag_in.at[2], 2, 1, n, 0, chunks) + product(ag_in.at[2], 2, 0, n, 0, chunks - 1)
    landed(ag_in.at[2, 0], af_rs.at[2])
    for n in range(parts):
        mixed_ref[:, n * step : (n + 1) * step] = (acc[n] + product(ag_in.at[2], 2, 0, n, chunks - 1, chunks)).astype(BF16)
    pair_info.wait_send()
    ahead.wait_send()
    for n, place in enumerate(
        (
            pair_out,
            w_buf.at[:3, :slab, :],
            tinfo.at[: nz - 1],
            t_buf.at[:, : nz - 1],
            yinfo.at[: ny - 1],
            y_in.at[:, : ny - 1],
            e_buf.at[:, : nz - 1],
            w_buf.at[:3, : ny * slab, :],
            w_buf.at[:3, : 2 * slab, :],
            w_buf.at[:3, :slab, :],
            ag_in.at[:2],
            f_out,
            ag_in.at[2],
        )
    ):
        left_here(place, group_ss.at[n])


def put_out(mixed_ref, gate_ref, mixed_hbm, gate_hbm, sems):
    copies = [pltpu.make_async_copy(mixed_ref, mixed_hbm, sems.at[0]), pltpu.make_async_copy(gate_ref, gate_hbm, sems.at[1])]
    for copy in copies:
        copy.start()
    for copy in copies:
        copy.wait()


def shards(queries, keys, values, forget_gate, input_gate, out_weight):
    tokens, heads = forget_gate.shape
    dk, dv = queries.shape[1] // heads, values.shape[1] // heads
    width = out_weight.shape[1]
    ny, nz, nx = (lax.axis_size(a) for a in ("y", "z", "x"))
    cols = width // nx
    share = dk // nz
    chunks, step = 4, 256
    wide = dv // chunks
    any_space = pl.BlockSpec(memory_space=pltpu.HBM)
    dma = pltpu.SemaphoreType.DMA
    info = lambda n: pltpu.VMEM((n, 1, INFO), F32)
    mixed, gate_mean = pl.pallas_call(
        functools.partial(kernel, (ny, nz, nx)),
        out_shape=(pltpu.VMEM((tokens, cols), BF16), pltpu.VMEM((1, heads), F32)),
        in_specs=[any_space] * 6,
        out_specs=(pl.BlockSpec(memory_space=pltpu.VMEM), pl.BlockSpec(memory_space=pltpu.VMEM)),
        scratch_shapes=[
            pltpu.VMEM((2, tokens, dk), BF16),
            pltpu.VMEM((2, tokens, dk), BF16),
            pltpu.VMEM((2, tokens, dv), BF16),
            pltpu.VMEM((heads, tokens), F32),
            pltpu.VMEM((heads, tokens), F32),
            pltpu.VMEM((4, heads * dv, cols), BF16),
            pltpu.VMEM((2, dk, tokens), BF16),
            pltpu.VMEM((2, dk, tokens), BF16),
            pltpu.VMEM((tokens, tokens), BF16),
            pltpu.VMEM((chunks, dk, wide), F32),
            pltpu.VMEM((chunks, dk, wide), BF16),
            pltpu.VMEM((chunks, dk, wide), BF16),
            info(1),
            info(1),
            pltpu.VMEM((chunks, nz, share, wide), BF16),
            pltpu.VMEM((chunks, nz, share, wide), BF16),
            info(1),
            info(nz),
            pltpu.VMEM((chunks, nz, share, wide), F32),
            pltpu.VMEM((chunks, share, wide), BF16),
            pltpu.VMEM((chunks, ny, share, wide), BF16),
            info(1),
            info(ny),
            pltpu.VMEM((chunks, nz, share, wide), BF16),
            pltpu.VMEM((chunks, nz, share, wide), BF16),
            pltpu.VMEM((chunks, dk, wide), BF16),
            pltpu.VMEM((chunks, dk, wide), BF16),
            info(1),
            info(1),
            pltpu.VMEM((chunks, dk, wide), BF16),
            pltpu.VMEM((2, tokens, dv), F32),
            pltpu.VMEM((2, tokens, 1), F32),
            pltpu.VMEM((2, tokens, 1), F32),
            pltpu.VMEM((2 * chunks, tokens, wide), BF16),
            pltpu.VMEM((3, 2 * chunks, tokens, wide), BF16),
            pltpu.VMEM((cols // step, tokens, step), F32),
            dma((8,)), dma((1,)),
            dma((2,)), dma((2,)), dma((13,)), dma((5,)),
            dma((chunks,)), dma((chunks,)), dma((chunks,)), dma((chunks,)), dma((chunks,)),
            dma((2, 3)), dma((2, 2 * chunks)), dma((3,)),
        ],
        compiler_params=pltpu.CompilerParams(
            collective_id=0, has_side_effects=True, vmem_limit_bytes=65000000
        ),
        name="mlstm_layer",
    )(queries, keys, values, forget_gate.T, input_gate.T, out_weight)
    in_vmem = pl.BlockSpec(memory_space=pltpu.VMEM)
    mixed, gate_mean = pl.pallas_call(
        put_out,
        out_shape=(jax.ShapeDtypeStruct((tokens, cols), BF16), jax.ShapeDtypeStruct((1, heads), F32)),
        in_specs=[in_vmem, in_vmem],
        out_specs=(any_space, any_space),
        scratch_shapes=[dma((2,))],
        compiler_params=pltpu.CompilerParams(vmem_limit_bytes=4 * 1024 * 1024),
        name="put_out",
    )(mixed, gate_mean)
    return mixed, gate_mean.reshape(heads)


def solution(mesh):
    torus = Mesh(mesh.devices.reshape(4, 8, 2, mesh.shape["head"]), ("y", "z", "c", "x"))
    both = P(SEQ, "x")
    return jax.shard_map(
        shards,
        mesh=torus,
        in_specs=(both, both, both, both, both, P("x", None)),
        out_specs=(P(SEQ, "x"), P("x")),
        check_vma=False,
    )
```

```python
import functools

import jax
import jax.numpy as jnp
from jax import lax
from jax.experimental import pallas as pl
from jax.experimental.pallas import tpu as pltpu
from jax.sharding import Mesh
from jax.sharding import PartitionSpec as P

MESH = pl.DeviceIdType.MESH
SEQ = ("y", "z", "c")
F32 = jnp.float32
BF16 = jnp.bfloat16
LOW = -1e30
INFO = 384


def dot(a, b):
    return jnp.dot(a, b, preferred_element_type=F32)


def merge(e_max, l_max, l_decay):
    top = jnp.maximum(l_decay + e_max, l_max)
    return jnp.exp(l_decay + e_max - top), jnp.exp(l_max - top), top


def three_rows(row, first):
    hi = row.astype(BF16).astype(F32)
    mid = (row - hi).astype(BF16).astype(F32)
    low = row - hi - mid
    return jnp.where(first == 0, hi, jnp.where(first == 1, mid, jnp.where(first == 2, low, 0.0))).astype(BF16)


def read_info(ref, j):
    row = ref[j]
    return row[:, :256], row[:, 256:257], row[:, 288:289], row[:, 320:321]


def write_info(ref, norm, top, decay, gate):
    lane = lax.broadcasted_iota(jnp.int32, (1, 128), 1)
    ref[0, :, 0:256] = norm
    ref[0, :, 256:384] = jnp.where(lane < 32, top, jnp.where(lane < 64, decay, gate))


def kernel(
    sizes,
    q_hbm, k_hbm, v_hbm, fg_hbm, ig_hbm, w_hbm,
    mixed_ref, gate_ref,
    q_buf, k_buf, v_buf, fg_buf, ig_buf, w_buf, kt_buf, wkt_buf, upper,
    own1, pair_out, pair_in, pinfo_out, pinfo_in,
    t_buf, t_in, tinfo_out, tinfo,
    p_buf, y_out, y_in, yinfo_out, yinfo,
    e_buf, e_in, f_out, f_in, finfo_out, finfo_in, mine,
    num_buf, bmax_buf, den_buf, hid,
    ag_in, acc,
    load_sem, w_sem,
    one_ss, one_rs, group_ss, group_rs, pair_rs, z_rs, y_rs, e_rs, f_rs, wy_rs, ag_rs, af_rs,
):
    ny, nz, nx = sizes
    y, z, c, x = (lax.axis_index(a) for a in ("y", "z", "c", "x"))
    tokens = q_buf.shape[1]
    dk, dv = q_buf.shape[2], v_buf.shape[2]
    half = tokens // 2
    cols = w_buf.shape[2]
    slab = w_buf.shape[1] // (2 * ny)
    share = dk // nz
    chunks, wide, step = t_buf.shape[0], t_buf.shape[3], acc.shape[2]
    first = c == 0
    partner = {"c": 1 - c}
    heads = (1 - c, c)

    loads = []

    def load(src, dst):
        loads.append(pltpu.make_async_copy(src, dst, load_sem.at[len(loads)]))

    load(fg_hbm, fg_buf)
    load(ig_hbm, ig_buf)
    for s in range(2):
        load(k_hbm.at[:, pl.ds(pl.multiple_of(heads[s] * dk, 128), dk)], k_buf.at[s])
        load(v_hbm.at[:, pl.ds(pl.multiple_of(heads[s] * dv, 128), dv)], v_buf.at[s])
    for s in range(2):
        load(q_hbm.at[:, pl.ds(pl.multiple_of(heads[s] * dk, 128), dk)], q_buf.at[s])

    for copy in loads[:4]:
        copy.start()

    barrier = pltpu.get_barrier_semaphore()
    peers = [{"c": 1 - c}]
    peers += [{"z": lax.rem(z + d, nz)} for d in range(1, nz)]
    peers += [{"y": lax.rem(y + d, ny)} for d in range(1, ny)]
    left, right = {"x": lax.rem(x + nx - 1, nx)}, {"x": lax.rem(x + 1, nx)}
    far = {"x": lax.rem(x + 2, nx)}
    peers += [left, right, far]
    for peer in peers:
        pl.semaphore_signal(barrier, inc=1, device_id=peer, device_id_type=MESH)

    upper[...] = (
        (lax.broadcasted_iota(jnp.int32, (tokens, tokens), 0) <= lax.broadcasted_iota(jnp.int32, (tokens, tokens), 1))
        .astype(F32)
        .astype(BF16)
    )
    for copy in loads[:3]:
        copy.wait()
    for copy in loads[4:6]:
        copy.start()
    fg, ig = fg_buf[...], ig_buf[...]
    lf = jnp.minimum(fg, 0.0) - jnp.log1p(jnp.exp(-jnp.abs(fg)))
    lf_rows = (jnp.where(first, lf[1:2], lf[0:1]), jnp.where(first, lf[0:1], lf[1:2]))
    ig_rows = (jnp.where(first, ig[1:2], ig[0:1]), jnp.where(first, ig[0:1], ig[1:2]))
    sub = lax.broadcasted_iota(jnp.int32, (8, tokens), 0)
    stacked = jnp.where(
        sub < 4,
        three_rows(jnp.broadcast_to(lf_rows[0], (8, tokens)), sub).astype(F32),
        three_rows(jnp.broadcast_to(lf_rows[1], (8, tokens)), sub - 4).astype(F32),
    ).astype(BF16)
    cums = dot(stacked, upper[...])
    b_rows, decays, tops, weights = [], [], [], []
    for s in range(2):
        cum = jnp.sum(cums[4 * s : 4 * s + 4], axis=0, keepdims=True)
        b = ig_rows[s] - cum
        decay = cum[:, tokens - 1 : tokens]
        b_top = jnp.max(b, axis=1, keepdims=True)
        b_rows.append(b)
        decays.append(decay)
        tops.append(decay + b_top)
        weights.append(jnp.exp(b - b_top) * (dk**-0.5))
    gates = [jnp.sum(ig_rows[s], axis=1, keepdims=True) for s in range(2)]

    def own_keys(s):
        kt = k_buf[s].T
        kt_buf[s] = kt
        wkt_buf[s] = (kt.astype(F32) * weights[s]).astype(BF16)
        return jnp.sum(dot(three_rows(jnp.broadcast_to(weights[s], (8, tokens)), sub), k_buf[s]), axis=0, keepdims=True)

    def own_state(s, h):
        return dot(wkt_buf[s], v_buf[s, :, h * wide : (h + 1) * wide])

    def remote(src, dst, ss, rs, peer):
        return pltpu.make_async_remote_copy(
            src_ref=src, dst_ref=dst, send_sem=ss, recv_sem=rs, device_id=peer, device_id_type=MESH
        )

    def landed(place, sem):
        remote(place, place, sem, sem, partner).wait_recv()

    def left_here(place, sem):
        remote(place, place, sem, sem, partner).wait_send()

    norm0 = own_keys(0)
    write_info(pinfo_out, norm0, tops[0], decays[0], gates[0])
    loads[3].wait()
    for copy in loads[6:]:
        copy.start()
    pair_out[0] = own_state(0, 0).astype(BF16)
    pl.semaphore_wait(barrier, len(peers))
    pair_info = remote(pinfo_out, pinfo_in, one_ss.at[0], one_rs.at[0], partner)
    pair_info.start()
    pair = []

    def send_pair(h):
        copy = remote(pair_out.at[h], pair_in.at[h], group_ss.at[0], pair_rs.at[h], partner)
        copy.start()
        pair.append(copy)

    send_pair(0)
    for h in range(1, chunks):
        pair_out[h] = own_state(0, h).astype(BF16)
        send_pair(h)

    def slab_of(y_index, c_index):
        return pl.multiple_of((y_index * 2 + c_index) * slab, slab)

    mine_rows = pl.ds(slab_of(y, c), slab)
    for i, peer in ((0, right), (1, left), (2, far)):
        copy = remote(
            w_hbm.at[mine_rows, pl.ds(pl.multiple_of(peer["x"] * cols, 128), cols)], w_buf.at[i, mine_rows, :], group_ss.at[1], group_rs.at[0], peer
        )
        copy.start()
    w_own = pltpu.make_async_copy(w_hbm.at[:, pl.ds(pl.multiple_of(x * cols, 128), cols)], w_buf.at[3], w_sem.at[0])

    loads[4].wait()
    norm1 = own_keys(1)
    loads[5].wait()
    own1[0] = own_state(1, 0)

    pair_info.wait_recv()
    in_norm, in_top, in_decay, in_gate = read_info(pinfo_in, 0)
    a_top, a_norm = jnp.where(first, tops[1], in_top), jnp.where(first, norm1, in_norm)
    a_decay = jnp.where(first, decays[1], in_decay)
    l_top, l_norm = jnp.where(first, in_top, tops[1]), jnp.where(first, in_norm, norm1)
    l_decay = jnp.where(first, in_decay, decays[1])
    e_scale, l_scale, chip_top = merge(a_top, l_top, l_decay)
    chip_norm = e_scale * a_norm + l_scale * l_norm
    write_info(tinfo_out, chip_norm, chip_top, a_decay + l_decay, gates[1] + in_gate)
    order = sorted(range(1, nz), key=lambda d: -min(d, nz - d))
    for d in order:
        copy = remote(tinfo_out.at[0], tinfo.at[z], group_ss.at[3], group_rs.at[1], {"z": lax.rem(z + d, nz)})
        copy.start()
    tinfo[z] = tinfo_out[0]
    own_scale, in_scale = jnp.where(first, e_scale, l_scale), jnp.where(first, l_scale, e_scale)
    loads[6].wait()
    loads[7].wait()

    def intra(s):
        for r in range(2):
            rows = pl.ds(r * half, half)
            span = half * (r + 1)
            scores = dot(q_buf[s, rows, :], kt_buf[s, :, :span]) * (dk**-0.5)
            t_index = lax.broadcasted_iota(jnp.int32, (half, span), 0) + r * half
            s_index = lax.broadcasted_iota(jnp.int32, (half, span), 1)
            logs = jnp.where(s_index <= t_index, jnp.broadcast_to(b_rows[s][:, :span], (half, span)), -jnp.inf)
            top = jnp.max(logs, axis=1, keepdims=True)
            weighted = jnp.exp(logs - top) * scores
            bmax_buf[s, rows, :] = top
            den_buf[s, rows, :] = jnp.sum(weighted, axis=1, keepdims=True)
            num_buf[s, rows, :] = dot(weighted.astype(BF16), v_buf[s, :span, :])

    @pl.when(c == 0)
    def _():
        intra(1)

    for h in range(chunks):
        if h > 0:
            own1[h] = own_state(1, h)
        pair[h].wait_recv()
        for j in range(nz):
            rows = pl.ds(j * share, share)
            t_buf[h, j] = (own_scale * own1[h, rows, :] + in_scale * pair_in[h, rows, :].astype(F32)).astype(BF16)
        for d in order:
            peer = lax.rem(z + d, nz)
            copy = remote(t_buf.at[h, peer], t_in.at[h, z], group_ss.at[0], z_rs.at[h], {"z": peer})
            copy.start()
        t_in[h, z] = t_buf[h, z]

    w_own.start()

    @pl.when(c == 1)
    def _():
        intra(1)

    intra(0)

    landed(tinfo.at[: nz - 1], group_rs.at[1])
    top, decay, norm, gate = jnp.full((1, 1), LOW, F32), jnp.zeros((1, 1), F32), jnp.zeros((1, dk), F32), jnp.zeros((1, 1), F32)
    z_norm, z_top, z_decay = norm, top, decay
    z_tops, z_decays, scales = [], [], []
    for j in range(nz):
        z_tops.append(top)
        z_decays.append(decay)
        here = j == z
        z_norm, z_top, z_decay = jnp.where(here, norm, z_norm), jnp.where(here, top, z_top), jnp.where(here, decay, z_decay)
        j_norm, j_top, j_decay, j_gate = read_info(tinfo, j)
        e_scale, l_scale, top = merge(top, j_top, j_decay)
        norm = e_scale * norm + l_scale * j_norm
        decay = decay + j_decay
        gate = gate + j_gate
        scales.append((e_scale, l_scale))
    write_info(yinfo_out, norm, top, decay, gate)
    y_order = sorted(range(1, ny), key=lambda d: -min(d, ny - d))
    for d in y_order:
        copy = remote(yinfo_out.at[0], yinfo.at[y], group_ss.at[4], group_rs.at[2], {"y": lax.rem(y + d, ny)})
        copy.start()
    yinfo[y] = yinfo_out[0]
    for h in range(chunks):
        landed(t_in.at[h, : nz - 1], z_rs.at[h])
        running = jnp.zeros((share, wide), F32)
        for j in range(nz):
            p_buf[h, j] = running
            running = scales[j][0] * running + scales[j][1] * t_in[h, j].astype(F32)
        y_out[h] = running.astype(BF16)
        for d in y_order:
            copy = remote(y_out.at[h], y_in.at[h, y], group_ss.at[0], y_rs.at[h], {"y": lax.rem(y + d, ny)})
            copy.start()
        y_in[h, y] = y_out[h]

    landed(yinfo.at[: ny - 1], group_rs.at[2])
    top, decay, norm, gate = jnp.full((1, 1), LOW, F32), jnp.zeros((1, 1), F32), jnp.zeros((1, dk), F32), jnp.zeros((1, 1), F32)
    y_scales = []
    for j in range(ny):
        j_norm, j_top, j_decay, j_gate = read_info(yinfo, j)
        passed = j < y
        e_scale, l_scale, next_top = merge(top, j_top, j_decay)
        norm = jnp.where(passed, e_scale * norm + l_scale * j_norm, norm)
        top = jnp.where(passed, next_top, top)
        gate = gate + j_gate
        y_scales.append((jnp.where(passed, e_scale, 1.0), jnp.where(passed, l_scale, 0.0)))
    e_scales = [merge(top, z_tops[j], z_decays[j]) for j in range(nz)]
    e_scale, l_scale, chip_max = merge(top, z_top, z_decay)
    enter_norm = e_scale * norm + l_scale * z_norm

    e_scale, l_scale, both_max = merge(chip_max, a_top, a_decay)
    both_norm = e_scale * enter_norm + l_scale * a_norm
    my_max, my_norm = jnp.where(first, chip_max, both_max), jnp.where(first, enter_norm, both_norm)
    write_info(finfo_out, jnp.where(first, both_norm, enter_norm), jnp.where(first, both_max, chip_max), a_decay, gate)
    ahead = remote(finfo_out, finfo_in, one_ss.at[1], one_rs.at[1], partner)
    ahead.start()

    def factors(s, norm, top):
        for r in range(2):
            rows = pl.ds(r * half, half)
            carried_den = jnp.sum(q_buf[s, rows, :].astype(F32) * norm, axis=1, keepdims=True)
            b_top = bmax_buf[s, rows, :]
            stabilizer = jnp.maximum(b_top, top)
            a, k = jnp.exp(b_top - stabilizer), jnp.exp(top - stabilizer)
            den = a * den_buf[s, rows, :] + k * carried_den
            inverse = 1.0 / jnp.maximum(jnp.abs(den), 1.0)
            bmax_buf[s, rows, :] = a * inverse
            den_buf[s, rows, :] = k * inverse

    for h in range(chunks):
        landed(y_in.at[h, : ny - 1], y_rs.at[h])
        before = jnp.zeros((share, wide), F32)
        for j in range(ny):
            before = y_scales[j][0] * before + y_scales[j][1] * y_in[h, j].astype(F32)
        for j in range(nz):
            e_buf[h, j] = (e_scales[j][0] * before + e_scales[j][1] * p_buf[h, j]).astype(BF16)
        for d in order:
            peer = lax.rem(z + d, nz)
            copy = remote(e_buf.at[h, peer], e_in.at[h, z], group_ss.at[0], e_rs.at[h], {"z": peer})
            copy.start()
        e_in[h, z] = e_buf[h, z]
        if h == 0:
            factors(1, my_norm, my_max)
        if h == chunks - 2:
            ahead.wait_recv()
            other_norm, other_max, unused_decay, other_gate = read_info(finfo_in, 0)
            factors(0, other_norm, other_max)

    upward, downward = {"y": lax.rem(y + 1, ny)}, {"y": lax.rem(y + ny - 1, ny)}
    def to_partner(i, rows):
        place = w_buf.at[i, rows, :]
        remote(place, place, group_ss.at[1], group_rs.at[3], partner).start()

    def start_weights():
        landed(w_buf.at[:3, :slab, :], group_rs.at[0])
        for i in range(3):
            place = w_buf.at[i, mine_rows, :]
            for peer in (upward, downward):
                remote(place, place, group_ss.at[1], wy_rs.at[i], peer).start()
            to_partner(i, mine_rows)

    def pass_weights(i):
        landed(w_buf.at[i, : 2 * slab, :], wy_rs.at[i])
        for way, peer, source in ((0, upward, y + ny - 1), (1, downward, y + 1)):
            start = slab_of(lax.rem(source, ny), c)
            place = w_buf.at[i, pl.ds(pl.multiple_of(start + way * (slab // 2), slab // 2), slab // 2), :]
            copy = remote(place, place, group_ss.at[1], group_rs.at[4], peer)
            copy.start()
            to_partner(i, pl.ds(start, slab))

    lane = lax.broadcasted_iota(jnp.int32, (1, 2), 1)
    gate_ref[...] = jnp.where(lane == c, gate, other_gate) * (1.0 / (tokens * ny * nz * 2))

    def readout(s, h, carry):
        for r in range(2):
            rows = pl.ds(r * half, half)
            carried = dot(q_buf[s, rows, :], carry)
            own = num_buf[s, rows, h * wide : (h + 1) * wide]
            hid[s * chunks + h, rows, :] = (bmax_buf[s, rows, :] * own + den_buf[s, rows, :] * carried).astype(BF16)

    sequence = []

    def gather(s, h):
        r = s * chunks + h
        sequence.append(r)
        for way, peer in ((0, right), (1, left)):
            copy = remote(hid.at[r], ag_in.at[way, r], group_ss.at[2], ag_rs.at[r], peer)
            copy.start()

    finish = []
    for h in range(chunks):
        landed(e_in.at[h, : nz - 1], e_rs.at[h])
        for j in range(nz):
            rows = pl.ds(j * share, share)
            entering = e_in[h, j].astype(F32)
            a_rows = jnp.where(first, own1[h, rows, :], pair_in[h, rows, :].astype(F32))
            both = e_scale * entering + l_scale * a_rows
            f_out[h, rows, :] = jnp.where(first, both, entering).astype(BF16)
            mine[h, rows, :] = jnp.where(first, entering, both).astype(BF16)
        copy = remote(f_out.at[h], f_in.at[h], group_ss.at[0], f_rs.at[h], partner)
        copy.start()
        finish.append(copy)
        readout(1, h, mine[h])
        gather(1, h)
        if h == 0:
            start_weights()
        if h > 0:
            finish[h - 1].wait_recv()
            readout(0, h - 1, f_in[h - 1])
            gather(0, h - 1)
    finish[chunks - 1].wait_recv()
    readout(0, chunks - 1, f_in[chunks - 1])
    gather(0, chunks - 1)

    def product(source, i, s, n, low, high):
        hidden = [source[s * chunks + h] for h in range(low, high)]
        left_side = hidden[0] if len(hidden) == 1 else jnp.concatenate(hidden, axis=1)
        rows = pl.ds(pl.multiple_of(heads[s] * dv + low * wide, wide), (high - low) * wide)
        return dot(left_side, w_buf[i, rows, n * step : (n + 1) * step])

    parts = cols // step
    w_own.wait()
    for n in range(parts):
        acc[n] = product(hid, 3, 1, n, 0, chunks) + product(hid, 3, 0, n, 0, chunks)

    last = chunks - 1

    def pass_hidden(r):
        group = 0 if r >= chunks else 2 if r == last else 1
        landed(ag_in.at[:2, r], ag_rs.at[r])
        for way, peer in ((0, right), (1, left)):
            rows = pl.ds(way * half, half)
            copy = remote(ag_in.at[way, r, rows, :], ag_in.at[2, r, rows, :], group_ss.at[2], af_rs.at[group], peer)
            copy.start()

    plan = iter(sequence)
    for i, count in ((0, 1), (1, 2), (2, 2)):
        for _ in range(count):
            pass_hidden(next(plan))
        pass_weights(i)
    for r in plan:
        pass_hidden(r)
    far_rows = pl.ds(slab_of(lax.rem(y + 2, ny), c), slab)
    landed(w_buf.at[:3, :slab, :], group_rs.at[4])
    for i in range(3):
        to_partner(i, far_rows)
    landed(w_buf.at[:3, : ny * slab, :], group_rs.at[3])
    for n in range(parts):
        acc[n] += (product(ag_in.at[0], 0, 1, n, 0, chunks) + product(ag_in.at[0], 0, 0, n, 0, chunks)) + (
            product(ag_in.at[1], 1, 1, n, 0, chunks) + product(ag_in.at[1], 1, 0, n, 0, chunks)
        )

    landed(ag_in.at[2, :chunks], af_rs.at[0])
    landed(ag_in.at[2, :last], af_rs.at[1])
    for n in range(parts):
        acc[n] += product(ag_in.at[2], 2, 1, n, 0, chunks) + product(ag_in.at[2], 2, 0, n, 0, chunks - 1)
    landed(ag_in.at[2, 0], af_rs.at[2])
    for n in range(parts):
        mixed_ref[:, n * step : (n + 1) * step] = (acc[n] + product(ag_in.at[2], 2, 0, n, chunks - 1, chunks)).astype(BF16)
    pair_info.wait_send()
    ahead.wait_send()
    state_rows = (2 * dk * dv + 2 * (nz - 1) * share * dv + (ny - 1) * share * dv) // cols
    for n, place in enumerate((w_buf.at[0, :state_rows, :], w_buf.at[:3], ag_in, tinfo.at[: nz - 1], yinfo.at[: ny - 1])):
        left_here(place, group_ss.at[n])


def put_out(mixed_ref, gate_ref, mixed_hbm, gate_hbm, sems):
    copies = [pltpu.make_async_copy(mixed_ref, mixed_hbm, sems.at[0]), pltpu.make_async_copy(gate_ref, gate_hbm, sems.at[1])]
    for copy in copies:
        copy.start()
    for copy in copies:
        copy.wait()


def shards(queries, keys, values, forget_gate, input_gate, out_weight):
    tokens, heads = forget_gate.shape
    dk, dv = queries.shape[1] // heads, values.shape[1] // heads
    width = out_weight.shape[1]
    ny, nz, nx = (lax.axis_size(a) for a in ("y", "z", "x"))
    cols = width // nx
    share = dk // nz
    chunks, step = 4, 256
    wide = dv // chunks
    any_space = pl.BlockSpec(memory_space=pltpu.HBM)
    dma = pltpu.SemaphoreType.DMA
    info = lambda n: pltpu.VMEM((n, 1, INFO), F32)
    mixed, gate_mean = pl.pallas_call(
        functools.partial(kernel, (ny, nz, nx)),
        out_shape=(pltpu.VMEM((tokens, cols), BF16), pltpu.VMEM((1, heads), F32)),
        in_specs=[any_space] * 6,
        out_specs=(pl.BlockSpec(memory_space=pltpu.VMEM), pl.BlockSpec(memory_space=pltpu.VMEM)),
        scratch_shapes=[
            pltpu.VMEM((2, tokens, dk), BF16),
            pltpu.VMEM((2, tokens, dk), BF16),
            pltpu.VMEM((2, tokens, dv), BF16),
            pltpu.VMEM((heads, tokens), F32),
            pltpu.VMEM((heads, tokens), F32),
            pltpu.VMEM((4, heads * dv, cols), BF16),
            pltpu.VMEM((2, dk, tokens), BF16),
            pltpu.VMEM((2, dk, tokens), BF16),
            pltpu.VMEM((tokens, tokens), BF16),
            pltpu.VMEM((chunks, dk, wide), F32),
            pltpu.VMEM((chunks, dk, wide), BF16),
            pltpu.VMEM((chunks, dk, wide), BF16),
            info(1),
            info(1),
            pltpu.VMEM((chunks, nz, share, wide), BF16),
            pltpu.VMEM((chunks, nz, share, wide), BF16),
            info(1),
            info(nz),
            pltpu.VMEM((chunks, nz, share, wide), F32),
            pltpu.VMEM((chunks, share, wide), BF16),
            pltpu.VMEM((chunks, ny, share, wide), BF16),
            info(1),
            info(ny),
            pltpu.VMEM((chunks, nz, share, wide), BF16),
            pltpu.VMEM((chunks, nz, share, wide), BF16),
            pltpu.VMEM((chunks, dk, wide), BF16),
            pltpu.VMEM((chunks, dk, wide), BF16),
            info(1),
            info(1),
            pltpu.VMEM((chunks, dk, wide), BF16),
            pltpu.VMEM((2, tokens, dv), F32),
            pltpu.VMEM((2, tokens, 1), F32),
            pltpu.VMEM((2, tokens, 1), F32),
            pltpu.VMEM((2 * chunks, tokens, wide), BF16),
            pltpu.VMEM((3, 2 * chunks, tokens, wide), BF16),
            pltpu.VMEM((cols // step, tokens, step), F32),
            dma((8,)), dma((1,)),
            dma((2,)), dma((2,)), dma((5,)), dma((5,)),
            dma((chunks,)), dma((chunks,)), dma((chunks,)), dma((chunks,)), dma((chunks,)),
            dma((3,)), dma((2 * chunks,)), dma((3,)),
        ],
        compiler_params=pltpu.CompilerParams(
            collective_id=0, has_side_effects=True, vmem_limit_bytes=65000000
        ),
        name="mlstm_layer",
    )(queries, keys, values, forget_gate.T, input_gate.T, out_weight)
    in_vmem = pl.BlockSpec(memory_space=pltpu.VMEM)
    mixed, gate_mean = pl.pallas_call(
        put_out,
        out_shape=(jax.ShapeDtypeStruct((tokens, cols), BF16), jax.ShapeDtypeStruct((1, heads), F32)),
        in_specs=[in_vmem, in_vmem],
        out_specs=(any_space, any_space),
        scratch_shapes=[dma((2,))],
        compiler_params=pltpu.CompilerParams(vmem_limit_bytes=4 * 1024 * 1024),
        name="put_out",
    )(mixed, gate_mean)
    return mixed, gate_mean.reshape(heads)


def solution(mesh):
    torus = Mesh(mesh.devices.reshape(4, 8, 2, mesh.shape["head"]), ("y", "z", "c", "x"))
    both = P(SEQ, "x")
    return jax.shard_map(
        shards,
        mesh=torus,
        in_specs=(both, both, both, both, both, P("x", None)),
        out_specs=(P(SEQ, "x"), P("x")),
        check_vma=False,
    )
```

```python
import functools

import jax
import jax.numpy as jnp
from jax import lax
from jax.experimental import pallas as pl
from jax.experimental.pallas import tpu as pltpu
from jax.sharding import Mesh
from jax.sharding import PartitionSpec as P

MESH = pl.DeviceIdType.MESH
SEQ = ("y", "z", "c")
F32 = jnp.float32
BF16 = jnp.bfloat16
LOW = -1e30
INFO = 384


def dot(a, b):
    return jnp.dot(a, b, preferred_element_type=F32)


def merge(e_max, l_max, l_decay):
    top = jnp.maximum(l_decay + e_max, l_max)
    return jnp.exp(l_decay + e_max - top), jnp.exp(l_max - top), top


def three_rows(row, first):
    hi = row.astype(BF16).astype(F32)
    mid = (row - hi).astype(BF16).astype(F32)
    low = row - hi - mid
    return jnp.where(first == 0, hi, jnp.where(first == 1, mid, jnp.where(first == 2, low, 0.0))).astype(BF16)


def read_info(ref, j):
    row = ref[j]
    return row[:, :256], row[:, 256:257], row[:, 288:289], row[:, 320:321]


def write_info(ref, norm, top, decay, gate):
    lane = lax.broadcasted_iota(jnp.int32, (1, 128), 1)
    ref[0, :, 0:256] = norm
    ref[0, :, 256:384] = jnp.where(lane < 32, top, jnp.where(lane < 64, decay, gate))


def kernel(
    sizes,
    q_hbm, k_hbm, v_hbm, fg_hbm, ig_hbm, w_hbm,
    mixed_ref, gate_ref,
    q_buf, k_buf, v_buf, fg_buf, ig_buf, w_buf, kt_buf, wkt_buf, upper,
    own1, pair_out, pair_in, pinfo_out, pinfo_in,
    t_buf, t_in, tinfo_out, tinfo,
    p_buf, y_out, y_in, yinfo_out, yinfo,
    e_buf, e_in, f_out, f_in, finfo_out, finfo_in, mine,
    num_buf, bmax_buf, den_buf, hid,
    ag_in, acc,
    load_sem, w_sem,
    one_ss, one_rs, group_ss, group_rs, pair_rs, z_rs, y_rs, e_rs, f_rs, wy_rs, ag_rs, af_rs,
):
    ny, nz, nx = sizes
    y, z, c, x = (lax.axis_index(a) for a in ("y", "z", "c", "x"))
    tokens = q_buf.shape[1]
    dk, dv = q_buf.shape[2], v_buf.shape[2]
    half = tokens // 2
    cols = w_buf.shape[2]
    slab = w_buf.shape[1] // (2 * ny)
    share = dk // nz
    chunks, wide, step = t_buf.shape[0], t_buf.shape[3], acc.shape[2]
    first = c == 0
    partner = {"c": 1 - c}
    heads = (1 - c, c)

    loads = []

    def load(src, dst):
        loads.append(pltpu.make_async_copy(src, dst, load_sem.at[len(loads)]))

    load(fg_hbm, fg_buf)
    load(ig_hbm, ig_buf)
    for s in range(2):
        load(k_hbm.at[:, pl.ds(pl.multiple_of(heads[s] * dk, 128), dk)], k_buf.at[s])
        load(v_hbm.at[:, pl.ds(pl.multiple_of(heads[s] * dv, 128), dv)], v_buf.at[s])
    for s in range(2):
        load(q_hbm.at[:, pl.ds(pl.multiple_of(heads[s] * dk, 128), dk)], q_buf.at[s])

    for copy in loads[:4]:
        copy.start()

    barrier = pltpu.get_barrier_semaphore()
    peers = [{"c": 1 - c}]
    peers += [{"z": lax.rem(z + d, nz)} for d in range(1, nz)]
    peers += [{"y": lax.rem(y + d, ny)} for d in range(1, ny)]
    left, right = {"x": lax.rem(x + nx - 1, nx)}, {"x": lax.rem(x + 1, nx)}
    far = {"x": lax.rem(x + 2, nx)}
    peers += [left, right, far]
    for peer in peers:
        pl.semaphore_signal(barrier, inc=1, device_id=peer, device_id_type=MESH)

    upper[...] = (
        (lax.broadcasted_iota(jnp.int32, (tokens, tokens), 0) <= lax.broadcasted_iota(jnp.int32, (tokens, tokens), 1))
        .astype(F32)
        .astype(BF16)
    )
    for copy in loads[:3]:
        copy.wait()
    for copy in loads[4:6]:
        copy.start()
    fg, ig = fg_buf[...], ig_buf[...]
    lf = jnp.minimum(fg, 0.0) - jnp.log1p(jnp.exp(-jnp.abs(fg)))
    lf_rows = (jnp.where(first, lf[1:2], lf[0:1]), jnp.where(first, lf[0:1], lf[1:2]))
    ig_rows = (jnp.where(first, ig[1:2], ig[0:1]), jnp.where(first, ig[0:1], ig[1:2]))
    sub = lax.broadcasted_iota(jnp.int32, (8, tokens), 0)
    stacked = jnp.where(
        sub < 4,
        three_rows(jnp.broadcast_to(lf_rows[0], (8, tokens)), sub).astype(F32),
        three_rows(jnp.broadcast_to(lf_rows[1], (8, tokens)), sub - 4).astype(F32),
    ).astype(BF16)
    cums = dot(stacked, upper[...])
    b_rows, decays, tops, weights = [], [], [], []
    for s in range(2):
        cum = jnp.sum(cums[4 * s : 4 * s + 4], axis=0, keepdims=True)
        b = ig_rows[s] - cum
        decay = cum[:, tokens - 1 : tokens]
        b_top = jnp.max(b, axis=1, keepdims=True)
        b_rows.append(b)
        decays.append(decay)
        tops.append(decay + b_top)
        weights.append(jnp.exp(b - b_top) * (dk**-0.5))
    gates = [jnp.sum(ig_rows[s], axis=1, keepdims=True) for s in range(2)]

    def own_keys(s):
        kt = k_buf[s].T
        kt_buf[s] = kt
        wkt_buf[s] = (kt.astype(F32) * weights[s]).astype(BF16)
        return jnp.sum(dot(three_rows(jnp.broadcast_to(weights[s], (8, tokens)), sub), k_buf[s]), axis=0, keepdims=True)

    def own_state(s, h):
        return dot(wkt_buf[s], v_buf[s, :, h * wide : (h + 1) * wide])

    def remote(src, dst, ss, rs, peer):
        return pltpu.make_async_remote_copy(
            src_ref=src, dst_ref=dst, send_sem=ss, recv_sem=rs, device_id=peer, device_id_type=MESH
        )

    def landed(place, sem):
        remote(place, place, sem, sem, partner).wait_recv()

    def left_here(place, sem):
        remote(place, place, sem, sem, partner).wait_send()

    norm0 = own_keys(0)
    write_info(pinfo_out, norm0, tops[0], decays[0], gates[0])
    loads[3].wait()
    for copy in loads[6:]:
        copy.start()
    pair_out[0] = own_state(0, 0).astype(BF16)
    pl.semaphore_wait(barrier, len(peers))
    pair_info = remote(pinfo_out, pinfo_in, one_ss.at[0], one_rs.at[0], partner)
    pair_info.start()
    pair = []

    def send_pair(h):
        copy = remote(pair_out.at[h], pair_in.at[h], group_ss.at[0], pair_rs.at[h], partner)
        copy.start()
        pair.append(copy)

    send_pair(0)
    for h in range(1, chunks):
        pair_out[h] = own_state(0, h).astype(BF16)
        send_pair(h)

    def slab_of(y_index, c_index):
        return pl.multiple_of((y_index * 2 + c_index) * slab, slab)

    mine_rows = pl.ds(slab_of(y, c), slab)
    for i, peer in ((0, right), (1, left), (2, far)):
        copy = remote(
            w_hbm.at[mine_rows, pl.ds(pl.multiple_of(peer["x"] * cols, 128), cols)], w_buf.at[i, mine_rows, :], group_ss.at[1], group_rs.at[0], peer
        )
        copy.start()
    w_own = pltpu.make_async_copy(w_hbm.at[:, pl.ds(pl.multiple_of(x * cols, 128), cols)], w_buf.at[3], w_sem.at[0])

    loads[4].wait()
    norm1 = own_keys(1)
    loads[5].wait()
    own1[0] = own_state(1, 0)

    pair_info.wait_recv()
    in_norm, in_top, in_decay, in_gate = read_info(pinfo_in, 0)
    a_top, a_norm = jnp.where(first, tops[1], in_top), jnp.where(first, norm1, in_norm)
    a_decay = jnp.where(first, decays[1], in_decay)
    l_top, l_norm = jnp.where(first, in_top, tops[1]), jnp.where(first, in_norm, norm1)
    l_decay = jnp.where(first, in_decay, decays[1])
    e_scale, l_scale, chip_top = merge(a_top, l_top, l_decay)
    chip_norm = e_scale * a_norm + l_scale * l_norm
    write_info(tinfo_out, chip_norm, chip_top, a_decay + l_decay, gates[1] + in_gate)
    order = sorted(range(1, nz), key=lambda d: (-min(d, nz - d), -d))
    for d in order:
        copy = remote(tinfo_out.at[0], tinfo.at[z], group_ss.at[3], group_rs.at[1], {"z": lax.rem(z + d, nz)})
        copy.start()
    tinfo[z] = tinfo_out[0]
    own_scale, in_scale = jnp.where(first, e_scale, l_scale), jnp.where(first, l_scale, e_scale)
    loads[6].wait()
    loads[7].wait()

    def intra(s):
        for r in range(2):
            rows = pl.ds(r * half, half)
            span = half * (r + 1)
            scores = dot(q_buf[s, rows, :], kt_buf[s, :, :span]) * (dk**-0.5)
            t_index = lax.broadcasted_iota(jnp.int32, (half, span), 0) + r * half
            s_index = lax.broadcasted_iota(jnp.int32, (half, span), 1)
            logs = jnp.where(s_index <= t_index, jnp.broadcast_to(b_rows[s][:, :span], (half, span)), -jnp.inf)
            top = jnp.max(logs, axis=1, keepdims=True)
            weighted = jnp.exp(logs - top) * scores
            bmax_buf[s, rows, :] = top
            den_buf[s, rows, :] = jnp.sum(weighted, axis=1, keepdims=True)
            num_buf[s, rows, :] = dot(weighted.astype(BF16), v_buf[s, :span, :])

    @pl.when(c == 0)
    def _():
        intra(1)

    for h in range(chunks):
        if h > 0:
            own1[h] = own_state(1, h)
        pair[h].wait_recv()
        for j in range(nz):
            rows = pl.ds(j * share, share)
            t_buf[h, j] = (own_scale * own1[h, rows, :] + in_scale * pair_in[h, rows, :].astype(F32)).astype(BF16)
        for d in order:
            peer = lax.rem(z + d, nz)
            copy = remote(t_buf.at[h, peer], t_in.at[h, z], group_ss.at[0], z_rs.at[h], {"z": peer})
            copy.start()
        t_in[h, z] = t_buf[h, z]

    w_own.start()

    @pl.when(c == 1)
    def _():
        intra(1)

    intra(0)

    landed(tinfo.at[: nz - 1], group_rs.at[1])
    top, decay, norm, gate = jnp.full((1, 1), LOW, F32), jnp.zeros((1, 1), F32), jnp.zeros((1, dk), F32), jnp.zeros((1, 1), F32)
    z_norm, z_top, z_decay = norm, top, decay
    z_tops, z_decays, scales = [], [], []
    for j in range(nz):
        z_tops.append(top)
        z_decays.append(decay)
        here = j == z
        z_norm, z_top, z_decay = jnp.where(here, norm, z_norm), jnp.where(here, top, z_top), jnp.where(here, decay, z_decay)
        j_norm, j_top, j_decay, j_gate = read_info(tinfo, j)
        e_scale, l_scale, top = merge(top, j_top, j_decay)
        norm = e_scale * norm + l_scale * j_norm
        decay = decay + j_decay
        gate = gate + j_gate
        scales.append((e_scale, l_scale))
    write_info(yinfo_out, norm, top, decay, gate)
    y_order = sorted(range(1, ny), key=lambda d: -min(d, ny - d))
    for d in y_order:
        copy = remote(yinfo_out.at[0], yinfo.at[y], group_ss.at[4], group_rs.at[2], {"y": lax.rem(y + d, ny)})
        copy.start()
    yinfo[y] = yinfo_out[0]
    for h in range(chunks):
        landed(t_in.at[h, : nz - 1], z_rs.at[h])
        running = jnp.zeros((share, wide), F32)
        for j in range(nz):
            p_buf[h, j] = running
            running = scales[j][0] * running + scales[j][1] * t_in[h, j].astype(F32)
        y_out[h] = running.astype(BF16)
        for d in y_order:
            copy = remote(y_out.at[h], y_in.at[h, y], group_ss.at[0], y_rs.at[h], {"y": lax.rem(y + d, ny)})
            copy.start()
        y_in[h, y] = y_out[h]

    landed(yinfo.at[: ny - 1], group_rs.at[2])
    top, decay, norm, gate = jnp.full((1, 1), LOW, F32), jnp.zeros((1, 1), F32), jnp.zeros((1, dk), F32), jnp.zeros((1, 1), F32)
    y_scales = []
    for j in range(ny):
        j_norm, j_top, j_decay, j_gate = read_info(yinfo, j)
        passed = j < y
        e_scale, l_scale, next_top = merge(top, j_top, j_decay)
        norm = jnp.where(passed, e_scale * norm + l_scale * j_norm, norm)
        top = jnp.where(passed, next_top, top)
        gate = gate + j_gate
        y_scales.append((jnp.where(passed, e_scale, 1.0), jnp.where(passed, l_scale, 0.0)))
    e_scales = [merge(top, z_tops[j], z_decays[j]) for j in range(nz)]
    e_scale, l_scale, chip_max = merge(top, z_top, z_decay)
    enter_norm = e_scale * norm + l_scale * z_norm

    e_scale, l_scale, both_max = merge(chip_max, a_top, a_decay)
    both_norm = e_scale * enter_norm + l_scale * a_norm
    my_max, my_norm = jnp.where(first, chip_max, both_max), jnp.where(first, enter_norm, both_norm)
    write_info(finfo_out, jnp.where(first, both_norm, enter_norm), jnp.where(first, both_max, chip_max), a_decay, gate)
    ahead = remote(finfo_out, finfo_in, one_ss.at[1], one_rs.at[1], partner)
    ahead.start()

    def factors(s, norm, top):
        for r in range(2):
            rows = pl.ds(r * half, half)
            carried_den = jnp.sum(q_buf[s, rows, :].astype(F32) * norm, axis=1, keepdims=True)
            b_top = bmax_buf[s, rows, :]
            stabilizer = jnp.maximum(b_top, top)
            a, k = jnp.exp(b_top - stabilizer), jnp.exp(top - stabilizer)
            den = a * den_buf[s, rows, :] + k * carried_den
            inverse = 1.0 / jnp.maximum(jnp.abs(den), 1.0)
            bmax_buf[s, rows, :] = a * inverse
            den_buf[s, rows, :] = k * inverse

    for h in range(chunks):
        landed(y_in.at[h, : ny - 1], y_rs.at[h])
        before = jnp.zeros((share, wide), F32)
        for j in range(ny):
            before = y_scales[j][0] * before + y_scales[j][1] * y_in[h, j].astype(F32)
        for j in range(nz):
            e_buf[h, j] = (e_scales[j][0] * before + e_scales[j][1] * p_buf[h, j]).astype(BF16)
        for d in order:
            peer = lax.rem(z + d, nz)
            copy = remote(e_buf.at[h, peer], e_in.at[h, z], group_ss.at[0], e_rs.at[h], {"z": peer})
            copy.start()
        e_in[h, z] = e_buf[h, z]
        if h == 0:
            factors(1, my_norm, my_max)
        if h == chunks - 2:
            ahead.wait_recv()
            other_norm, other_max, unused_decay, other_gate = read_info(finfo_in, 0)
            factors(0, other_norm, other_max)

    upward, downward = {"y": lax.rem(y + 1, ny)}, {"y": lax.rem(y + ny - 1, ny)}
    def to_partner(i, rows):
        place = w_buf.at[i, rows, :]
        remote(place, place, group_ss.at[1], group_rs.at[3], partner).start()

    def start_weights():
        landed(w_buf.at[:3, :slab, :], group_rs.at[0])
        for i in range(3):
            place = w_buf.at[i, mine_rows, :]
            for peer in (upward, downward):
                remote(place, place, group_ss.at[1], wy_rs.at[i], peer).start()
            to_partner(i, mine_rows)

    def pass_weights(i):
        landed(w_buf.at[i, : 2 * slab, :], wy_rs.at[i])
        for way, peer, source in ((0, upward, y + ny - 1), (1, downward, y + 1)):
            start = slab_of(lax.rem(source, ny), c)
            place = w_buf.at[i, pl.ds(pl.multiple_of(start + way * (slab // 2), slab // 2), slab // 2), :]
            copy = remote(place, place, group_ss.at[1], group_rs.at[4], peer)
            copy.start()
            to_partner(i, pl.ds(start, slab))

    lane = lax.broadcasted_iota(jnp.int32, (1, 2), 1)
    gate_ref[...] = jnp.where(lane == c, gate, other_gate) * (1.0 / (tokens * ny * nz * 2))

    def readout(s, h, carry):
        for r in range(2):
            rows = pl.ds(r * half, half)
            carried = dot(q_buf[s, rows, :], carry)
            own = num_buf[s, rows, h * wide : (h + 1) * wide]
            hid[s * chunks + h, rows, :] = (bmax_buf[s, rows, :] * own + den_buf[s, rows, :] * carried).astype(BF16)

    sequence = []

    def gather(s, h):
        r = s * chunks + h
        sequence.append(r)
        for way, peer in ((0, right), (1, left)):
            copy = remote(hid.at[r], ag_in.at[way, r], group_ss.at[2], ag_rs.at[r], peer)
            copy.start()

    finish = []
    for h in range(chunks):
        landed(e_in.at[h, : nz - 1], e_rs.at[h])
        for j in range(nz):
            rows = pl.ds(j * share, share)
            entering = e_in[h, j].astype(F32)
            mine[h, rows, :] = jnp.where(first, entering, e_scale * entering + l_scale * pair_in[h, rows, :].astype(F32)).astype(BF16)
        readout(1, h, mine[h])
        gather(1, h)
        for j in range(nz):
            rows = pl.ds(j * share, share)
            entering = e_in[h, j].astype(F32)
            f_out[h, rows, :] = jnp.where(first, e_scale * entering + l_scale * own1[h, rows, :], entering).astype(BF16)
        copy = remote(f_out.at[h], f_in.at[h], group_ss.at[0], f_rs.at[h], partner)
        copy.start()
        finish.append(copy)
        if h == 0:
            start_weights()
        if h > 0:
            finish[h - 1].wait_recv()
            readout(0, h - 1, f_in[h - 1])
            gather(0, h - 1)
    finish[chunks - 1].wait_recv()
    readout(0, chunks - 1, f_in[chunks - 1])
    gather(0, chunks - 1)

    def product(source, i, s, n, low, high):
        hidden = [source[s * chunks + h] for h in range(low, high)]
        left_side = hidden[0] if len(hidden) == 1 else jnp.concatenate(hidden, axis=1)
        rows = pl.ds(pl.multiple_of(heads[s] * dv + low * wide, wide), (high - low) * wide)
        return dot(left_side, w_buf[i, rows, n * step : (n + 1) * step])

    parts = cols // step
    w_own.wait()
    for n in range(parts):
        acc[n] = product(hid, 3, 1, n, 0, chunks) + product(hid, 3, 0, n, 0, chunks)

    last = chunks - 1

    def pass_hidden(r):
        group = 0 if r >= chunks else 2 if r == last else 1
        landed(ag_in.at[:2, r], ag_rs.at[r])
        for way, peer in ((0, right), (1, left)):
            rows = pl.ds(way * half, half)
            copy = remote(ag_in.at[way, r, rows, :], ag_in.at[2, r, rows, :], group_ss.at[2], af_rs.at[group], peer)
            copy.start()

    plan = iter(sequence)
    for i, count in ((0, 1), (1, 2), (2, 2)):
        for _ in range(count):
            pass_hidden(next(plan))
        pass_weights(i)
    for r in plan:
        pass_hidden(r)
    far_rows = pl.ds(slab_of(lax.rem(y + 2, ny), c), slab)
    landed(w_buf.at[:3, :slab, :], group_rs.at[4])
    for i in range(3):
        to_partner(i, far_rows)
    landed(w_buf.at[:3, : ny * slab, :], group_rs.at[3])
    for n in range(parts):
        acc[n] += (product(ag_in.at[0], 0, 1, n, 0, chunks) + product(ag_in.at[0], 0, 0, n, 0, chunks)) + (
            product(ag_in.at[1], 1, 1, n, 0, chunks) + product(ag_in.at[1], 1, 0, n, 0, chunks)
        )

    landed(ag_in.at[2, :chunks], af_rs.at[0])
    landed(ag_in.at[2, :last], af_rs.at[1])
    for n in range(parts):
        acc[n] += product(ag_in.at[2], 2, 1, n, 0, chunks) + product(ag_in.at[2], 2, 0, n, 0, chunks - 1)
    landed(ag_in.at[2, 0], af_rs.at[2])
    for n in range(parts):
        mixed_ref[:, n * step : (n + 1) * step] = (acc[n] + product(ag_in.at[2], 2, 0, n, chunks - 1, chunks)).astype(BF16)
    pair_info.wait_send()
    ahead.wait_send()
    state_rows = (2 * dk * dv + 2 * (nz - 1) * share * dv + (ny - 1) * share * dv) // cols
    for n, place in enumerate((w_buf.at[0, :state_rows, :], w_buf.at[:3], ag_in, tinfo.at[: nz - 1], yinfo.at[: ny - 1])):
        left_here(place, group_ss.at[n])


def put_out(mixed_ref, gate_ref, mixed_hbm, gate_hbm, sems):
    copies = [pltpu.make_async_copy(mixed_ref, mixed_hbm, sems.at[0]), pltpu.make_async_copy(gate_ref, gate_hbm, sems.at[1])]
    for copy in copies:
        copy.start()
    for copy in copies:
        copy.wait()


def shards(queries, keys, values, forget_gate, input_gate, out_weight):
    tokens, heads = forget_gate.shape
    dk, dv = queries.shape[1] // heads, values.shape[1] // heads
    width = out_weight.shape[1]
    ny, nz, nx = (lax.axis_size(a) for a in ("y", "z", "x"))
    cols = width // nx
    share = dk // nz
    chunks, step = 4, 256
    wide = dv // chunks
    any_space = pl.BlockSpec(memory_space=pltpu.HBM)
    dma = pltpu.SemaphoreType.DMA
    info = lambda n: pltpu.VMEM((n, 1, INFO), F32)
    mixed, gate_mean = pl.pallas_call(
        functools.partial(kernel, (ny, nz, nx)),
        out_shape=(pltpu.VMEM((tokens, cols), BF16), pltpu.VMEM((1, heads), F32)),
        in_specs=[any_space] * 6,
        out_specs=(pl.BlockSpec(memory_space=pltpu.VMEM), pl.BlockSpec(memory_space=pltpu.VMEM)),
        scratch_shapes=[
            pltpu.VMEM((2, tokens, dk), BF16),
            pltpu.VMEM((2, tokens, dk), BF16),
            pltpu.VMEM((2, tokens, dv), BF16),
            pltpu.VMEM((heads, tokens), F32),
            pltpu.VMEM((heads, tokens), F32),
            pltpu.VMEM((4, heads * dv, cols), BF16),
            pltpu.VMEM((2, dk, tokens), BF16),
            pltpu.VMEM((2, dk, tokens), BF16),
            pltpu.VMEM((tokens, tokens), BF16),
            pltpu.VMEM((chunks, dk, wide), F32),
            pltpu.VMEM((chunks, dk, wide), BF16),
            pltpu.VMEM((chunks, dk, wide), BF16),
            info(1),
            info(1),
            pltpu.VMEM((chunks, nz, share, wide), BF16),
            pltpu.VMEM((chunks, nz, share, wide), BF16),
            info(1),
            info(nz),
            pltpu.VMEM((chunks, nz, share, wide), F32),
            pltpu.VMEM((chunks, share, wide), BF16),
            pltpu.VMEM((chunks, ny, share, wide), BF16),
            info(1),
            info(ny),
            pltpu.VMEM((chunks, nz, share, wide), BF16),
            pltpu.VMEM((chunks, nz, share, wide), BF16),
            pltpu.VMEM((chunks, dk, wide), BF16),
            pltpu.VMEM((chunks, dk, wide), BF16),
            info(1),
            info(1),
            pltpu.VMEM((chunks, dk, wide), BF16),
            pltpu.VMEM((2, tokens, dv), F32),
            pltpu.VMEM((2, tokens, 1), F32),
            pltpu.VMEM((2, tokens, 1), F32),
            pltpu.VMEM((2 * chunks, tokens, wide), BF16),
            pltpu.VMEM((3, 2 * chunks, tokens, wide), BF16),
            pltpu.VMEM((cols // step, tokens, step), F32),
            dma((8,)), dma((1,)),
            dma((2,)), dma((2,)), dma((5,)), dma((5,)),
            dma((chunks,)), dma((chunks,)), dma((chunks,)), dma((chunks,)), dma((chunks,)),
            dma((3,)), dma((2 * chunks,)), dma((3,)),
        ],
        compiler_params=pltpu.CompilerParams(
            collective_id=0, has_side_effects=True, vmem_limit_bytes=65000000
        ),
        name="mlstm_layer",
    )(queries, keys, values, forget_gate.T, input_gate.T, out_weight)
    in_vmem = pl.BlockSpec(memory_space=pltpu.VMEM)
    mixed, gate_mean = pl.pallas_call(
        put_out,
        out_shape=(jax.ShapeDtypeStruct((tokens, cols), BF16), jax.ShapeDtypeStruct((1, heads), F32)),
        in_specs=[in_vmem, in_vmem],
        out_specs=(any_space, any_space),
        scratch_shapes=[dma((2,))],
        compiler_params=pltpu.CompilerParams(vmem_limit_bytes=4 * 1024 * 1024),
        name="put_out",
    )(mixed, gate_mean)
    return mixed, gate_mean.reshape(heads)


def solution(mesh):
    torus = Mesh(mesh.devices.reshape(4, 8, 2, mesh.shape["head"]), ("y", "z", "c", "x"))
    both = P(SEQ, "x")
    return jax.shard_map(
        shards,
        mesh=torus,
        in_specs=(both, both, both, both, both, P("x", None)),
        out_specs=(P(SEQ, "x"), P("x")),
        check_vma=False,
    )
```
